512 devices in a mesh: groups: 2 (over y), tensor: 32 (over z, core), section: 8 (over x).
Axes of the slice: x: 8, y: 2, z: 16, core: 2. Of those that a mesh axis runs over, the one named last changes fastest.
The devices are a block of a 8x8x16 slice.
Arguments:
- hidden: bfloat16 [128, 8192], P('groups', 'tensor'), parts along dimension 0, may hold values from -6 to 6
- norm_gain: bfloat16 [8, 8192], P('section'), may hold values from 0.5 to 1.5
- query_weight: bfloat16 [8, 8192, 4096], P('section', None, 'tensor'), may hold values from -0.0625 to 0.0625
- query_bias: bfloat16 [8, 4096], P('section', 'tensor'), may hold values from -10 to 10
- kv_weight: bfloat16 [8, 8192, 1024], P('section', None, 'tensor'), may hold values from -0.0625 to 0.0625
- out_weight: bfloat16 [8, 4096, 8192], P('section', None, 'tensor'), may hold values from -0.09375 to 0.09375
- kv_pool: bfloat16 [8, 384, 16, 1024], P('section', ('groups', 'tensor')), parts along dimension 1, may hold values from -8 to 8
- page_table: int32 [128, 4], P(('groups', 'tensor')), parts along dimension 0, may hold values from 0 to 191, as said below
- context_len: int32 [128], P(('groups', 'tensor')), parts along dimension 0, may hold values from 33 to 64, as said below
Outputs:
- result: bfloat16 [128, 8192], P(('groups', 'section'), 'tensor'), parts along dimension 0
The draws below stay inside these ranges and needn't reach their ends.
There are 2 independent parts, one for each index of `groups`. The reference program is written for one: setup_inputs(seed, part) draws one part's arguments, and reference() takes and returns one part's arrays. A program takes and returns all parts, laid end to end along the dimension named above; an argument that names none is the same for every part. Nothing has to cross between parts.
Inputs may be any that keep to these rules, and one draw needn't show every extreme that they name: `page_table`: sample r belongs to block k = r // 2; its 4 pages lie in k * 6 to (k + 1) * 6 - 1. The first 2 pages are the same for all samples of a block, every other page belongs to one sample only. `context_len`: some sample has 64 cached tokens.
All inputs are finite; a program needn't handle non-finite values.
Results may differ from the reference program's by a relative error of at most 0.018.
Values may be sent and summed in bfloat16 or wider, within the bound.
A program may use at most 64 MiB of HBM per device.

```python
import jax
import jax.numpy as jnp
from jax import lax

D = 8192
HD = 128
HEADS = 32
KVH = 4
LAYERS = 8
ROW_DEV = 2
ROWS = 64
PAGE_LEN = 16
BLOCKS = 4
PREFIX_BLOCKS = 2
CTX = 64
POOL_DEV = 6
PAGES = 192
N_TENSOR = 32


def device_order(sub_key):
    return jax.random.permutation(sub_key, POOL_DEV).astype(jnp.int32)


def draw_page_table(key, part):
    orders = jax.vmap(device_order)(jax.random.split(jax.random.fold_in(key, 11), N_TENSOR))
    shared = jnp.broadcast_to(orders[:, None, :PREFIX_BLOCKS], (N_TENSOR, ROW_DEV, PREFIX_BLOCKS))
    private = orders[:, PREFIX_BLOCKS:].reshape(N_TENSOR, ROW_DEV, BLOCKS - PREFIX_BLOCKS)
    offsets = (jnp.arange(N_TENSOR, dtype=jnp.int32) * POOL_DEV)[:, None, None]
    table = jnp.concatenate([shared, private], axis=2) + offsets
    return table.reshape(ROWS, BLOCKS).astype(jnp.int32)


def draw_context_len(key, part):
    lowest = PREFIX_BLOCKS * PAGE_LEN + 1
    highest = BLOCKS * PAGE_LEN
    drawn = jax.random.randint(jax.random.fold_in(key, 23), (ROWS,), lowest, highest + 1, dtype=jnp.int32)
    marked = jax.random.randint(jax.random.fold_in(key, 29), (), 0, ROWS, dtype=jnp.int32)
    return jnp.where(jnp.arange(ROWS, dtype=jnp.int32) == marked, highest, drawn).astype(jnp.int32)


def draw_kv_pool(key, part):
    shape = (LAYERS, PAGES, PAGE_LEN, 2 * KVH * HD)
    base = jnp.clip(jax.random.normal(jax.random.fold_in(key, 31), shape, jnp.float32), -6.0, 6.0)
    return base.astype(jnp.bfloat16)


def draw_query_bias(key, part):
    shape = (LAYERS, HEADS * HD)
    base = jnp.clip(jax.random.normal(jax.random.fold_in(key, 43), shape, jnp.float32), -4.0, 4.0)
    return base.astype(jnp.bfloat16)


def level_of(rng, extent, shards, low, high):
    level, own = 1.0, jax.random.fold_in(rng, 6)
    for dim, parts in shards:
        steps = jnp.exp(jax.random.uniform(jax.random.fold_in(own, dim), (parts,), jnp.float32, low / len(shards), high / len(shards)))
        level = level * jnp.repeat(steps, extent[dim] // parts).reshape([-1 if axis == dim else 1 for axis in range(len(extent))])
    return level


def normal_values(key, extent, width, most, cuts=(), kind=jnp.bfloat16):
    level = level_of(key, extent, cuts, -0.22, 0.18) if cuts else 1.0
    values = jax.random.normal(key, extent, jnp.float32) * width * level
    return jnp.minimum(jnp.maximum(values, -most), most).astype(kind)


def setup_inputs(seed: int = 0, part: int = 0) -> dict:
    arg_keys = jax.random.split(jax.random.key(seed), 10)
    part_splits = jax.random.split(jax.random.fold_in(arg_keys[9], part), 10)
    return {
        "hidden": normal_values(part_splits[0], (ROWS, D), 1.0, 6.0, ((1, 32),)),
        "norm_gain": jnp.clip(1.0 + 0.1 * jax.random.normal(arg_keys[1], (LAYERS, D), jnp.float32), 0.5, 1.5).astype(jnp.bfloat16),
        "query_weight": normal_values(arg_keys[2], (LAYERS, D, HEADS * HD), D ** -0.5, 0.0625, ((0, 8), (2, 32))),
        "query_bias": draw_query_bias(jax.random.fold_in(arg_keys[9], 71), part),
        "kv_weight": normal_values(arg_keys[4], (LAYERS, D, 2 * KVH * HD), D ** -0.5, 0.0625, ((0, 8), (2, 32))),
        "out_weight": normal_values(arg_keys[5], (LAYERS, HEADS * HD, D), (HEADS * HD) ** -0.5, 0.09375, ((0, 8), (2, 32))),
        "kv_pool": draw_kv_pool(jax.random.fold_in(jax.random.fold_in(arg_keys[9], part), 71), part),
        "page_table": draw_page_table(jax.random.fold_in(jax.random.fold_in(arg_keys[9], part), 71), part),
        "context_len": draw_context_len(jax.random.fold_in(jax.random.fold_in(arg_keys[9], part), 71), part),
    }


epsilon = 1e-06
rope_base = 1000000.0

def rotate(values, position):
    head_size = values.shape[-1]
    half_size = head_size // 2
    frequency = rope_base ** (-(jnp.arange(half_size, dtype=jnp.float32) * 2.0) / head_size)
    angles = position.astype(jnp.float32)[:, None] * frequency[None, :]
    cosine = jnp.cos(angles)[:, None, :]
    sine_part = jnp.sin(angles)[:, None, :]
    front_half = values[..., :half_size]
    back_half = values[..., half_size:]
    return jnp.concatenate([front_half * cosine - back_half * sine_part, back_half * cosine + front_half * sine_part], axis=-1)

def attend(queries, key_new, value_new, cached, position):
    row_count, head_count, head_size = queries.shape
    kv_heads = key_new.shape[1]
    group_size = head_count // kv_heads
    span_len = cached.shape[1]
    keys_all = cached[:, :, :kv_heads * head_size].reshape(row_count, span_len, kv_heads, head_size).astype(jnp.float32)
    values_all = cached[:, :, kv_heads * head_size:].reshape(row_count, span_len, kv_heads, head_size).astype(jnp.float32)
    grouped = queries.reshape(row_count, kv_heads, group_size, head_size).astype(jnp.float32)
    scaling = head_size ** (-0.5)
    scores = jnp.einsum('rkgd,rskd->rkgs', grouped, keys_all) * scaling
    own_score = jnp.einsum('rkgd,rkd->rkg', grouped, key_new.astype(jnp.float32)) * scaling
    usable = (jnp.arange(span_len, dtype=jnp.int32)[None, :] < position[:, None])[:, None, None, :]
    row_max = jnp.maximum(lax.optimization_barrier(jnp.max(jnp.where(usable, scores, -1e+30), axis=-1)), own_score)
    weights = jnp.where(usable, jnp.exp(scores - row_max[..., None]), 0.0)
    own_weight = jnp.exp(own_score - row_max)
    denominator = lax.optimization_barrier(jnp.sum(weights, axis=-1)) + own_weight
    weights = (weights / denominator[..., None]).astype(jnp.bfloat16)
    own_weight = (own_weight / denominator).astype(jnp.bfloat16)
    mixture = jnp.einsum('rkgs,rskd->rkgd', weights.astype(jnp.float32), values_all)
    mixture = mixture + own_weight.astype(jnp.float32)[..., None] * value_new.astype(jnp.float32)[:, :, None, :]
    return mixture.reshape(row_count, head_count * head_size).astype(jnp.bfloat16)

def reference(hidden, norm_gain, query_weight, query_bias, kv_weight, out_weight, kv_pool, page_table, context_len):
    stream = hidden
    for layer_index in range(LAYERS):
        wide_rows = stream.astype(jnp.float32)
        mean_sq = lax.optimization_barrier(jnp.mean(wide_rows * wide_rows, axis=1, keepdims=True))
        normed = (wide_rows * lax.rsqrt(mean_sq + epsilon) * norm_gain[layer_index].astype(jnp.float32)).astype(jnp.bfloat16)
        queries = (jnp.dot(normed, query_weight[layer_index], preferred_element_type=jnp.float32) + query_bias[layer_index].astype(jnp.float32)).astype(jnp.bfloat16)
        fresh_kv = jnp.dot(normed, kv_weight[layer_index], preferred_element_type=jnp.float32).astype(jnp.bfloat16)
        cached = kv_pool[layer_index][page_table].reshape(ROWS, CTX, 2 * KVH * HD)
        rotated = rotate(queries.reshape(ROWS, HEADS, HD).astype(jnp.float32), context_len).astype(jnp.bfloat16)
        key_new = rotate(fresh_kv[:, :KVH * HD].reshape(ROWS, KVH, HD).astype(jnp.float32), context_len).astype(jnp.bfloat16)
        value_new = fresh_kv[:, KVH * HD:].reshape(ROWS, KVH, HD)
        mixture = attend(rotated, key_new, value_new, cached, context_len)
        stream = (wide_rows + jnp.dot(mixture, out_weight[layer_index], preferred_element_type=jnp.float32)).astype(jnp.bfloat16)
    return stream
```

```python
import functools

import jax
import jax.numpy as jnp
from jax import lax
from jax.experimental import pallas as pl
from jax.experimental.pallas import tpu as pltpu
from jax.sharding import PartitionSpec as P

MESH = pl.DeviceIdType.MESH
EPSILON = 1e-06
LOG_ROPE_BASE = 13.815510557964274
BF16 = jnp.bfloat16
F32 = jnp.float32


def relay_tree(half):
    far = half // 2
    return {d: 0 if d <= far else far for d in range(1, half + 1)}


def kernel(
    nc,
    nsec,
    hidden_hbm,
    gain_hbm,
    wq_hbm,
    bias_hbm,
    wkv_hbm,
    wo_hbm,
    pool_hbm,
    table_ref,
    len_ref,
    out_ref,
    hid,
    gain_in,
    gain,
    wq,
    bias,
    wkv,
    wo,
    pool,
    keys,
    values,
    cos_tab,
    sin_tab,
    lim_tab,
    first,
    xbuf,
    qkv_out,
    qkv_in,
    mix_own,
    mixbuf,
    stream,
    load_sems,
    push_send,
    push_recv,
    x_send,
    x_recv,
    i_send,
    r_send,
    a2a_send,
    a2a_recv,
    m_send,
    m_root,
    m_recv,
    out_send,
    out_recv,
    ready,
    turn,
):
    row_dev, blocks = table_ref.shape
    width = hid.shape[2]
    rows = nc * row_dev
    hd = keys.shape[1]
    heads = mix_own.shape[0]
    page_len = pool.shape[1]
    span = page_len * blocks
    wide = keys.shape[0]
    kvh = wide // row_dev // span
    per_chip = heads // nc
    part = wkv.shape[0]
    half = nc // 2
    parent = relay_tree(half)
    kids = {d: sorted((c for c in parent if parent[c] == d), reverse=True) for d in range(half + 1)}
    far = half // 2
    near = [(s, d) for d in range(far, 0, -1) for s in (1, -1)] + [(1, 0)]

    me = lax.axis_index("tensor")
    sec = lax.axis_index("section")
    z = me // 2
    core = lax.rem(me, 2)
    last = nsec - 1

    def dev(zz, s=None):
        where = {"tensor": lax.rem(zz + 2 * nc, nc) * 2 + core}
        if s is not None:
            where["section"] = s
        return where

    def put(src, dst, ssem, rsem, where):
        copy = pltpu.make_async_remote_copy(
            src_ref=src, dst_ref=dst, send_sem=ssem, recv_sem=rsem, device_id=where, device_id_type=MESH
        )
        copy.start()
        return copy

    def wait_for(ref, sem):
        pltpu.make_async_copy(ref, ref, sem).wait()

    def cut(ref, axis, c):
        n = ref.shape[axis] // 2
        at = pl.multiple_of(c * n, n)
        return ref.at[pl.ds(at, n)] if axis == 0 else ref.at[:, pl.ds(at, n)]

    def shares(c):
        return [hid.at[c], bias.at[c], cut(wq, 1, c), cut(wkv, 0, c), cut(wo, 1, c)]

    sources = [hidden_hbm, bias_hbm, wq_hbm, wkv_hbm, wo_hbm]

    def load(k, src, dst):
        copy = pltpu.make_async_copy(src, dst, load_sems.at[k])
        copy.start()
        return copy

    load_gain, load_pool = load(0, gain_hbm, gain_in), load(1, pool_hbm, pool)
    own_loads = [load(2 + k, src, dst) for k, (src, dst) in enumerate(zip(sources, shares(core)))]

    barrier = pltpu.get_barrier_semaphore()

    def greet(where):
        pl.semaphore_signal(barrier, inc=1, device_id=where, device_id_type=MESH)

    sibling = {"tensor": z * 2 + 1 - core}
    greet(sibling)

    @pl.loop(1, nc)
    def _(i):
        greet(dev(z + i))

    @pl.when(sec < last)
    def _():
        for s, d in near:
            greet(dev(z + s * d, sec + 1))

    @pl.when(sec > 0)
    def _():
        pl.semaphore_wait(barrier, nc + len(near))
        for s, d in near:
            pl.semaphore_signal(ready, inc=1, device_id=dev(z - s * d, sec - 1), device_id_type=MESH)

    @pl.when(sec == 0)
    def _():
        pl.semaphore_wait(barrier, nc)

    pushes = [
        put(src, dst, push_send.at[k], push_recv.at[k], sibling)
        for k, (src, dst) in enumerate(zip(sources, shares(core)))
    ]

    def send_stream(src, section, sems):
        return [
            put(src, xbuf.at[z], sems.at[k], x_recv.at[z], dev(z + s * d, section) if d else dev(z, section))
            for k, (s, d) in enumerate(near)
        ]

    own_loads[0].wait()
    wait_for(hid.at[0], push_recv.at[0])

    @pl.when(jnp.logical_and(sec == 0, core == 1))
    def _():
        pl.semaphore_wait(turn, 1)

    @pl.when(sec == 0)
    def _():
        whole = 2 * rows
        at = lax.broadcasted_iota(jnp.int32, (rows, whole), 0)
        col = lax.broadcasted_iota(jnp.int32, (rows, whole), 1)
        row = (at // row_dev * 2 + core) * row_dev + lax.rem(at, row_dev)
        pick = jnp.where(col == row, 1.0, 0.0).astype(BF16)
        for c in range(2):
            first[c] = jnp.dot(pick, hid[c], preferred_element_type=F32).astype(BF16)
        for k, (s, d) in enumerate(near):
            if d:
                put(first, xbuf.at[z], i_send.at[k], x_recv.at[z], dev(z + s * d))
            else:
                pltpu.make_async_copy(first, xbuf.at[z], x_recv.at[z]).start()

    load_gain.wait()
    for t in range(2 * nc):
        gain[t] = gain_in[:, t * width : (t + 1) * width].astype(F32)
    load_pool.wait()
    for r in range(row_dev):
        for b in range(blocks):
            page = pool[lax.rem(table_ref[r, b], pool.shape[0])]
            for k in range(kvh):
                at = (r * kvh + k) * span + b * page_len
                keys[at : at + page_len, :] = page[:, k * hd : (k + 1) * hd]
                values[at : at + page_len, :] = page[:, (kvh + k) * hd : (kvh + k + 1) * hd]

    q_rows = per_chip * rows
    lane = lax.broadcasted_iota(jnp.int32, (q_rows, hd), 1)
    sample = lax.rem(lax.broadcasted_iota(jnp.int32, (q_rows, hd), 0), row_dev)
    position = jnp.full((q_rows, hd), len_ref[0], jnp.int32)
    for r in range(1, row_dev):
        position = jnp.where(sample == r, len_ref[r], position)
    position = position.astype(F32)
    frequency = jnp.exp(lax.rem(lane, hd // 2).astype(F32) * (-2.0 * LOG_ROPE_BASE / hd))
    angle = position * frequency
    sine = jnp.sin(angle)
    cos_tab[...] = jnp.cos(angle)
    sin_tab[...] = jnp.where(lane < hd // 2, -sine, sine)
    lim_tab[...] = position
    for k in range(1, 4):
        own_loads[k].wait()
        wait_for(shares(0)[k], push_recv.at[k])

    def chip_at(d, s):
        return lax.rem(z - s * d + nc, nc)

    def in_half(ref, s):
        n = ref.shape[0] // 2
        return ref.at[pl.ds(0 if s == 1 else n, n)]

    def arrivals(known):
        at = dict(known)
        for d in sorted(parent):
            if d not in at:
                at[d] = at[parent[d]] + 1.7 + 0.6 * (d - parent[d])
        return at

    ring = [(d, s) for d in range(1, half) for s in (1, -1)] + [(half, 1)]

    def relay(place, recv, sems, items, skip, use):
        sent = []
        for _, d, s in sorted(items):
            chip = chip_at(d, s)
            block = place(chip)
            wait_for(block, recv.at[chip])
            for way in (1, -1) if d == 0 else (s,):
                for c in kids[d]:
                    if (d, c) not in skip:
                        piece = in_half(block, way) if c == half else block
                        sent.append(
                            put(piece, piece, sems.at[len(sent)], recv.at[chip], dev(z + way * (c - d)))
                        )
            use(chip)
        return sent

    sums = {
        "q": jnp.zeros((rows, per_chip * hd), F32),
        "kv": jnp.zeros((rows, part), F32),
        "squares": jnp.zeros((rows, width), F32),
    }

    def project(chip):
        parts = []
        for c in range(2):
            x = xbuf[chip, c].astype(F32)
            sums["squares"] += x * x
            parts.append((x * gain[chip * 2 + c]).astype(BF16))
        y = jnp.concatenate(parts, axis=1)
        at = pl.multiple_of(chip * 2 * width, 2 * width)
        sums["q"] += jnp.dot(y, wq[pl.ds(at, 2 * width), :], preferred_element_type=F32)
        sums["kv"] += lax.dot_general(
            y, wkv[:, pl.ds(at, 2 * width)], (((1,), (1,)), ((), ())), preferred_element_type=F32
        )

    due = arrivals({d: 1.7 + 0.6 * d for d in range(far + 1)})
    direct = {(0, d) for d in range(1, far + 1)}
    x_sent = relay(
        lambda c: xbuf.at[c], x_recv, x_send, [(due[d], d, s) for d, s in [(0, 1)] + ring], direct, project
    )

    @pl.when(jnp.logical_and(sec == 0, core == 0))
    def _():
        pl.semaphore_signal(turn, inc=1, device_id=sibling, device_id_type=MESH)

    def mine(ref, c):
        return ref.at[:, pl.ds(c * row_dev, row_dev)]

    scale = lax.rsqrt(jnp.sum(sums["squares"], axis=1, keepdims=True) / (2 * nc * width) + EPSILON)
    for i in range(per_chip):
        q = sums["q"][:, i * hd : (i + 1) * hd] * scale + bias[i].astype(F32)
        qkv_out[i] = q.astype(BF16)
    kv = (sums["kv"] * scale).astype(BF16).astype(F32)
    kv = jnp.concatenate([kv, jnp.zeros((rows, hd - part), F32)], axis=1)
    kv = pltpu.roll(kv, lax.rem(z, hd // part) * part, 1)
    qkv_out[per_chip] = kv.astype(BF16)

    @pl.loop(0, nc - 1)
    def _(i):
        c = lax.rem(z + half + (1 - 2 * lax.rem(i, 2)) * ((i + 1) // 2) + nc, nc)
        put(mine(qkv_out, c), mine(qkv_in, z), a2a_send, a2a_recv, dev(c))

    pltpu.make_async_copy(mine(qkv_out, z), mine(qkv_in, z), a2a_recv).start()

    def grid(shape, axis):
        return lax.broadcasted_iota(jnp.int32, shape, axis)

    group = heads // kvh
    q_of, c_of = grid((q_rows, wide), 0), grid((q_rows, wide), 1)
    key_head = (lax.rem(q_of, rows) // row_dev * per_chip + q_of // rows) // group
    matching = c_of // span == lax.rem(q_of, row_dev) * kvh + key_head
    usable = matching & (lax.rem(c_of, span).astype(F32) < lim_tab[:, :1])
    s_row, s_col = grid((q_rows, rows), 0), grid((q_rows, rows), 1)
    same = lax.rem(s_row, row_dev) == lax.rem(s_col, row_dev)
    source = s_col // row_dev // (hd // part)
    wanted = (lax.rem(s_row, rows) // row_dev * per_chip + s_row // rows) // group
    pick_key = jnp.where(same & (source == wanted), 1.0, 0.0).astype(BF16)
    pick_value = jnp.where(same & (source == wanted + kvh), 1.0, 0.0).astype(BF16)
    root = hd ** (-0.5)
    cos, sin = cos_tab[...], sin_tab[...]
    wait_for(qkv_in, a2a_recv)

    def rotate(v):
        return (v * cos + pltpu.roll(v, hd // 2, 1) * sin).astype(BF16)

    rotated = rotate(jnp.concatenate([qkv_in[i].astype(F32) for i in range(per_chip)], axis=0))
    fresh = qkv_in[per_chip]
    key_new = rotate(jnp.dot(pick_key, fresh, preferred_element_type=F32))
    value_new = jnp.dot(pick_value, fresh, preferred_element_type=F32)
    scores = lax.dot_general(rotated, keys[...], (((1,), (1,)), ((), ())), preferred_element_type=F32) * root
    own_score = jnp.sum(rotated.astype(F32) * key_new.astype(F32), axis=1, keepdims=True) * root
    top = jnp.maximum(jnp.max(jnp.where(usable, scores, -1e30), axis=1, keepdims=True), own_score)
    weights = jnp.where(usable, jnp.exp(scores - top), 0.0)
    own_weight = jnp.exp(own_score - top)
    total = jnp.sum(weights, axis=1, keepdims=True) + own_weight
    weights = (weights / total).astype(BF16)
    own_weight = (own_weight / total).astype(BF16).astype(F32)
    mixture = jnp.dot(weights, values[...], preferred_element_type=F32) + own_weight * value_new
    mix_own[...] = mixture.astype(BF16).reshape(heads, row_dev, hd)

    def mix_place(c):
        return mixbuf.at[:, c]

    m_sent = []
    for c in kids[0]:
        for s in (1, -1):
            m_sent.append(put(mix_own, mix_place(z), m_root.at[len(m_sent)], m_recv.at[z], dev(z + s * c)))
    pltpu.make_async_copy(mix_own, mix_place(z), m_recv.at[z]).start()
    due = arrivals({0: 0.0})
    m_sent += relay(mix_place, m_recv, m_send, [(due[d], d, s) for d, s in ring], {}, lambda c: None)
    wait_for(mix_place(z), m_recv.at[z])

    own_loads[4].wait()
    wait_for(shares(0)[4], push_recv.at[4])

    mixed = [mixbuf[i * nc + c].reshape(rows, hd) for c in range(nc) for i in range(per_chip)]
    change = jnp.dot(jnp.concatenate(mixed, axis=1), wo[...], preferred_element_type=F32)
    for c in range(2):
        x = xbuf[z, c].astype(F32)
        stream[c] = (x + change[:, c * width : (c + 1) * width]).astype(BF16)

    chips = nc // nsec

    @pl.when(sec < last)
    def _():
        pl.semaphore_wait(ready, len(near))
        for copy in send_stream(stream, sec + 1, r_send):
            copy.wait_send()

    @pl.when(sec == last)
    def _():
        def share(s, c, j):
            return (
                stream.at[c, pl.ds((s * chips + j) * row_dev, row_dev)],
                out_ref.at[pl.ds((j * 2 + core) * row_dev, row_dev)],
            )

        def sem_of(s, c, j):
            return out_send.at[(j * 2 + c) * nsec + s]

        for j in range(chips):
            for c in range(2):

                @pl.loop(0, last)
                def _(s):
                    put(*share(s, c, j), sem_of(s, c, j), out_recv, {"section": s, "tensor": z * 2 + c})

                @pl.when(core == c)
                def _():
                    pltpu.make_async_copy(*share(last, c, j), out_recv).start()

                @pl.when(core != c)
                def _():
                    put(*share(last, c, j), sem_of(last, c, j), out_recv, sibling)

        for j in range(chips):
            for c in range(2):

                @pl.loop(0, last)
                def _(s):
                    wait_for(stream.at[0, pl.ds(0, row_dev)], sem_of(s, c, j))

                @pl.when(core != c)
                def _():
                    wait_for(stream.at[0, pl.ds(0, row_dev)], sem_of(last, c, j))

    @pl.when(sec == 0)
    def _():
        for k, (s, d) in enumerate(near):
            if d:
                wait_for(first, i_send.at[k])

    others = pl.ds(0, rows - row_dev)
    wait_for(qkv_out.at[:, others], a2a_send)
    for copy in pushes + x_sent + m_sent:
        copy.wait_send()
    wait_for(out_ref, out_recv)


def solution(mesh):
    nc, nsec = mesh.shape["tensor"] // 2, mesh.shape["section"]

    def step(hidden, norm_gain, query_weight, query_bias, kv_weight, out_weight, kv_pool, page_table, context_len):
        all_rows, width = hidden.shape
        features, hd = query_weight.shape[1:]
        pages, page_len, kv_width = kv_pool.shape[1:]
        row_dev, blocks = page_table.shape
        part = 2 * kv_weight.shape[2]
        kvh = kv_width // (2 * hd)
        cached = row_dev * kvh * blocks * page_len
        heads = 2 * nc
        rows = all_rows // 2
        q_rows = rows * heads // nc
        anywhere = pl.BlockSpec(memory_space=pl.ANY)
        scalars = pl.BlockSpec(memory_space=pltpu.SMEM)
        dma = pltpu.SemaphoreType.DMA
        vmem = pltpu.VMEM
        return pl.pallas_call(
            functools.partial(kernel, nc, nsec),
            out_shape=jax.ShapeDtypeStruct((all_rows // nsec, width), BF16),
            in_specs=[anywhere] * 7 + [scalars] * 2,
            out_specs=pl.BlockSpec(memory_space=vmem),
            scratch_shapes=[
                vmem((2, all_rows, width), BF16),
                vmem((1, features), BF16),
                vmem((2 * nc, 1, width), F32),
                vmem((features, 2 * hd), BF16),
                vmem((2, 1, hd), BF16),
                vmem((part, features), BF16),
                vmem((heads * hd, 2 * width), BF16),
                vmem((pages, page_len, kv_width), BF16),
                vmem((cached, hd), BF16),
                vmem((cached, hd), BF16),
                vmem((q_rows, hd), F32),
                vmem((q_rows, hd), F32),
                vmem((q_rows, hd), F32),
                vmem((2, rows, width), BF16),
                vmem((nc, 2, rows, width), BF16),
                vmem((3, rows, hd), BF16),
                vmem((3, rows, hd), BF16),
                vmem((heads, row_dev, hd), BF16),
                vmem((heads, nc, row_dev, hd), BF16),
                vmem((2, rows, width), BF16),
                dma((7,)),
                dma((5,)),
                dma((5,)),
                dma((2 * nc,)),
                dma((nc,)),
                dma((nc,)),
                dma((nc,)),
                dma,
                dma,
                dma((2 * nc,)),
                dma((2 * nc,)),
                dma((nc,)),
                dma((2 * nc,)),
                dma,
                pltpu.SemaphoreType.REGULAR,
                pltpu.SemaphoreType.REGULAR,
            ],
            compiler_params=pltpu.CompilerParams(collective_id=0, has_side_effects=True),
        )(
            hidden,
            norm_gain,
            query_weight[0],
            query_bias,
            kv_weight[0].T,
            out_weight[0],
            kv_pool[0],
            page_table,
            context_len,
        )

    tensor = "tensor"
    return jax.shard_map(
        step,
        mesh=mesh,
        in_specs=(
            P("groups", tensor),
            P("section", None),
            P("section", None, tensor),
            P("section", tensor),
            P("section", None, tensor),
            P("section", None, tensor),
            P("section", ("groups", tensor), None, None),
            P(("groups", tensor), None),
            P(("groups", tensor)),
        ),
        out_specs=P(("groups", "section"), tensor),
        check_vma=False,
    )
```

```python
import functools

import jax
import jax.numpy as jnp
from jax import lax
from jax.experimental import pallas as pl
from jax.experimental.pallas import tpu as pltpu
from jax.sharding import PartitionSpec as P

MESH = pl.DeviceIdType.MESH
EPSILON = 1e-06
LOG_ROPE_BASE = 13.815510557964274
BF16 = jnp.bfloat16
F32 = jnp.float32


def relay_tree(half):
    far = half // 2
    return {d: 0 if d <= far else far for d in range(1, half + 1)}


def kernel(
    nc,
    nsec,
    hidden_hbm,
    gain_hbm,
    wq_hbm,
    bias_hbm,
    wkv_hbm,
    wo_hbm,
    pool_hbm,
    table_ref,
    len_ref,
    out_ref,
    hid,
    gain_in,
    gain,
    wq,
    bias,
    wkv,
    wo,
    pool,
    keys,
    values,
    cos_tab,
    sin_tab,
    lim_tab,
    first,
    xbuf,
    qkv_out,
    qkv_in,
    mix_own,
    mixbuf,
    stream,
    load_sems,
    push_send,
    push_recv,
    x_send,
    x_recv,
    i_send,
    r_send,
    a2a_send,
    a2a_recv,
    m_send,
    m_root,
    m_recv,
    out_send,
    out_recv,
    ready,
    turn,
):
    row_dev, blocks = table_ref.shape
    width = hid.shape[2]
    rows = nc * row_dev
    hd = keys.shape[1]
    heads = mix_own.shape[0]
    page_len = pool.shape[1]
    span = page_len * blocks
    wide = keys.shape[0]
    kvh = wide // row_dev // span
    per_chip = heads // nc
    part = wkv.shape[0]
    half = nc // 2
    parent = relay_tree(half)
    kids = {d: sorted((c for c in parent if parent[c] == d), reverse=True) for d in range(half + 1)}
    far = half // 2
    near = [(s, d) for d in range(far, 0, -1) for s in (1, -1)] + [(1, 0)]

    me = lax.axis_index("tensor")
    sec = lax.axis_index("section")
    z = me // 2
    core = lax.rem(me, 2)
    last = nsec - 1

    def dev(zz, s=None):
        where = {"tensor": lax.rem(zz + 2 * nc, nc) * 2 + core}
        if s is not None:
            where["section"] = s
        return where

    def put(src, dst, ssem, rsem, where):
        copy = pltpu.make_async_remote_copy(
            src_ref=src, dst_ref=dst, send_sem=ssem, recv_sem=rsem, device_id=where, device_id_type=MESH
        )
        copy.start()
        return copy

    def wait_for(ref, sem):
        pltpu.make_async_copy(ref, ref, sem).wait()

    def cut(ref, axis, c):
        n = ref.shape[axis] // 2
        at = pl.multiple_of(c * n, n)
        return ref.at[pl.ds(at, n)] if axis == 0 else ref.at[:, pl.ds(at, n)]

    def shares(c):
        return [hid.at[c], bias.at[c], cut(wq, 1, c), cut(wkv, 0, c), cut(wo, 1, c)]

    sources = [hidden_hbm, bias_hbm, wq_hbm, wkv_hbm, wo_hbm]

    def load(k, src, dst):
        copy = pltpu.make_async_copy(src, dst, load_sems.at[k])
        copy.start()
        return copy

    load_gain, load_pool = load(0, gain_hbm, gain_in), load(1, pool_hbm, pool)
    own_loads = [load(2 + k, src, dst) for k, (src, dst) in enumerate(zip(sources, shares(core)))]

    barrier = pltpu.get_barrier_semaphore()

    def greet(where):
        pl.semaphore_signal(barrier, inc=1, device_id=where, device_id_type=MESH)

    sibling = {"tensor": z * 2 + 1 - core}
    greet(sibling)

    @pl.loop(1, nc)
    def _(i):
        greet(dev(z + i))

    @pl.when(sec < last)
    def _():
        for s, d in near:
            greet(dev(z + s * d, sec + 1))

    @pl.when(sec > 0)
    def _():
        pl.semaphore_wait(barrier, nc + len(near))
        for s, d in near:
            pl.semaphore_signal(ready, inc=1, device_id=dev(z - s * d, sec - 1), device_id_type=MESH)

    @pl.when(sec == 0)
    def _():
        pl.semaphore_wait(barrier, nc)

    pushes = [
        put(src, dst, push_send.at[k], push_recv.at[k], sibling)
        for k, (src, dst) in enumerate(zip(sources, shares(core)))
    ]

    def send_stream(src, section, sems):
        return [
            put(src, xbuf.at[z], sems.at[k], x_recv.at[z], dev(z + s * d, section) if d else dev(z, section))
            for k, (s, d) in enumerate(near)
        ]

    own_loads[0].wait()
    wait_for(hid.at[0], push_recv.at[0])

    @pl.when(jnp.logical_and(sec == 0, core == 1))
    def _():
        pl.semaphore_wait(turn, 1)

    @pl.when(sec == 0)
    def _():
        whole = 2 * rows
        at = lax.broadcasted_iota(jnp.int32, (rows, whole), 0)
        col = lax.broadcasted_iota(jnp.int32, (rows, whole), 1)
        row = (at // row_dev * 2 + core) * row_dev + lax.rem(at, row_dev)
        pick = jnp.where(col == row, 1.0, 0.0).astype(BF16)
        for c in range(2):
            first[c] = jnp.dot(pick, hid[c], preferred_element_type=F32).astype(BF16)
        for k, (s, d) in enumerate(near):
            if d:
                put(first, xbuf.at[z], i_send.at[k], x_recv.at[z], dev(z + s * d))
            else:
                pltpu.make_async_copy(first, xbuf.at[z], x_recv.at[z]).start()

    load_gain.wait()
    for t in range(2 * nc):
        gain[t] = gain_in[:, t * width : (t + 1) * width].astype(F32)
    load_pool.wait()
    for r in range(row_dev):
        for b in range(blocks):
            page = pool[lax.rem(table_ref[r, b], pool.shape[0])]
            for k in range(kvh):
                at = (r * kvh + k) * span + b * page_len
                keys[at : at + page_len, :] = page[:, k * hd : (k + 1) * hd]
                values[at : at + page_len, :] = page[:, (kvh + k) * hd : (kvh + k + 1) * hd]

    q_rows = per_chip * rows
    lane = lax.broadcasted_iota(jnp.int32, (q_rows, hd), 1)
    sample = lax.rem(lax.broadcasted_iota(jnp.int32, (q_rows, hd), 0), row_dev)
    position = jnp.full((q_rows, hd), len_ref[0], jnp.int32)
    for r in range(1, row_dev):
        position = jnp.where(sample == r, len_ref[r], position)
    position = position.astype(F32)
    frequency = jnp.exp(lax.rem(lane, hd // 2).astype(F32) * (-2.0 * LOG_ROPE_BASE / hd))
    angle = position * frequency
    sine = jnp.sin(angle)
    cos_tab[...] = jnp.cos(angle)
    sin_tab[...] = jnp.where(lane < hd // 2, -sine, sine)
    lim_tab[...] = position
    for k in range(1, 4):
        own_loads[k].wait()
        wait_for(shares(0)[k], push_recv.at[k])

    def chip_at(d, s):
        return lax.rem(z - s * d + nc, nc)

    def in_half(ref, s):
        n = ref.shape[0] // 2
        return ref.at[pl.ds(0 if s == 1 else n, n)]

    ring = [(far, 1), (far, -1)]
    ring += [(d, s) for d in range(1, half) if d != far for s in (1, -1)] + [(half, 1)]

    def relay(place, recv, sems, items, direct, use):
        sent, passed = [], []
        for d, s in items:
            chip = chip_at(d, s)
            block = place(chip)
            wait_for(block, recv.at[chip])
            if d != far and passed:
                use(passed)
                passed = []
            passed.append(chip)
            for c in kids[d] if (d, s) not in direct else []:
                piece = in_half(block, s) if c == half else block
                sent.append(put(piece, piece, sems.at[len(sent)], recv.at[chip], dev(z + s * (c - d))))
        use(passed)
        return sent

    sums = {
        "q": jnp.zeros((rows, per_chip * hd), F32),
        "kv": jnp.zeros((rows, part), F32),
        "squares": jnp.zeros((rows, width), F32),
    }

    def project(chips):
        for chip in chips:
            project_one(chip)

    def project_one(chip):
        parts = []
        for c in range(2):
            x = xbuf[chip, c].astype(F32)
            sums["squares"] += x * x
            parts.append((x * gain[chip * 2 + c]).astype(BF16))
        y = jnp.concatenate(parts, axis=1)
        at = pl.multiple_of(chip * 2 * width, 2 * width)
        sums["q"] += jnp.dot(y, wq[pl.ds(at, 2 * width), :], preferred_element_type=F32)
        sums["kv"] += lax.dot_general(
            y, wkv[:, pl.ds(at, 2 * width)], (((1,), (1,)), ((), ())), preferred_element_type=F32
        )

    x_sent = relay(
        lambda c: xbuf.at[c], x_recv, x_send, ring[:2] + [(0, 1)] + ring[2:], [(0, 1)], project
    )

    @pl.when(jnp.logical_and(sec == 0, core == 0))
    def _():
        pl.semaphore_signal(turn, inc=1, device_id=sibling, device_id_type=MESH)

    def mine(ref, c):
        return ref.at[:, pl.ds(c * row_dev, row_dev)]

    scale = lax.rsqrt(jnp.sum(sums["squares"], axis=1, keepdims=True) / (2 * nc * width) + EPSILON)
    for i in range(per_chip):
        q = sums["q"][:, i * hd : (i + 1) * hd] * scale + bias[i].astype(F32)
        qkv_out[i] = q.astype(BF16)
    kv = (sums["kv"] * scale).astype(BF16).astype(F32)
    kv = jnp.concatenate([kv, jnp.zeros((rows, hd - part), F32)], axis=1)
    kv = pltpu.roll(kv, lax.rem(z, hd // part) * part, 1)
    qkv_out[per_chip] = kv.astype(BF16)

    for i in range(nc - 1):
        c = lax.rem(z + half + (1 - 2 * (i % 2)) * ((i + 1) // 2) + nc, nc)
        put(mine(qkv_out, c), mine(qkv_in, z), a2a_send, a2a_recv, dev(c))

    pltpu.make_async_copy(mine(qkv_out, z), mine(qkv_in, z), a2a_recv).start()

    def grid(shape, axis):
        return lax.broadcasted_iota(jnp.int32, shape, axis)

    group = heads // kvh
    q_of, c_of = grid((q_rows, wide), 0), grid((q_rows, wide), 1)
    key_head = (lax.rem(q_of, rows) // row_dev * per_chip + q_of // rows) // group
    matching = c_of // span == lax.rem(q_of, row_dev) * kvh + key_head
    usable = matching & (lax.rem(c_of, span).astype(F32) < lim_tab[:, :1])
    s_row, s_col = grid((q_rows, rows), 0), grid((q_rows, rows), 1)
    same = lax.rem(s_row, row_dev) == lax.rem(s_col, row_dev)
    source = s_col // row_dev // (hd // part)
    wanted = (lax.rem(s_row, rows) // row_dev * per_chip + s_row // rows) // group
    pick_key = jnp.where(same & (source == wanted), 1.0, 0.0).astype(BF16)
    pick_value = jnp.where(same & (source == wanted + kvh), 1.0, 0.0).astype(BF16)
    root = hd ** (-0.5)
    cos, sin = cos_tab[...], sin_tab[...]
    wait_for(qkv_in, a2a_recv)

    def rotate(v):
        return (v * cos + pltpu.roll(v, hd // 2, 1) * sin).astype(BF16)

    rotated = rotate(jnp.concatenate([qkv_in[i].astype(F32) for i in range(per_chip)], axis=0))
    fresh = qkv_in[per_chip]
    key_new = rotate(jnp.dot(pick_key, fresh, preferred_element_type=F32))
    value_new = jnp.dot(pick_value, fresh, preferred_element_type=F32)
    scores = lax.dot_general(rotated, keys[...], (((1,), (1,)), ((), ())), preferred_element_type=F32) * root
    own_score = jnp.sum(rotated.astype(F32) * key_new.astype(F32), axis=1, keepdims=True) * root
    top = jnp.maximum(jnp.max(jnp.where(usable, scores, -1e30), axis=1, keepdims=True), own_score)
    weights = jnp.where(usable, jnp.exp(scores - top), 0.0)
    own_weight = jnp.exp(own_score - top)
    total = jnp.sum(weights, axis=1, keepdims=True) + own_weight
    weights = (weights / total).astype(BF16)
    own_weight = (own_weight / total).astype(BF16).astype(F32)
    mixture = jnp.dot(weights, values[...], preferred_element_type=F32) + own_weight * value_new
    mix_own[...] = mixture.astype(BF16).reshape(heads, row_dev, hd)

    def mix_place(c):
        return mixbuf.at[:, c]

    m_sent = []
    for c in kids[0]:
        for s in (1, -1):
            m_sent.append(put(mix_own, mix_place(z), m_root.at[len(m_sent)], m_recv.at[z], dev(z + s * c)))
    pltpu.make_async_copy(mix_own, mix_place(z), m_recv.at[z]).start()
    m_sent += relay(mix_place, m_recv, m_send, ring, [], lambda chips: None)
    wait_for(mix_place(z), m_recv.at[z])

    own_loads[4].wait()
    wait_for(shares(0)[4], push_recv.at[4])

    mixed = [mixbuf[i * nc + c].reshape(rows, hd) for c in range(nc) for i in range(per_chip)]
    change = jnp.dot(jnp.concatenate(mixed, axis=1), wo[...], preferred_element_type=F32)
    for c in range(2):
        x = xbuf[z, c].astype(F32)
        stream[c] = (x + change[:, c * width : (c + 1) * width]).astype(BF16)

    chips = nc // nsec

    @pl.when(sec < last)
    def _():
        pl.semaphore_wait(ready, len(near))
        for copy in send_stream(stream, sec + 1, r_send):
            copy.wait_send()

    @pl.when(sec == last)
    def _():
        def share(s, c, j):
            return (
                stream.at[c, pl.ds((s * chips + j) * row_dev, row_dev)],
                out_ref.at[pl.ds((j * 2 + core) * row_dev, row_dev)],
            )

        def sem_of(s, c, j):
            return out_send.at[(j * 2 + c) * nsec + s]

        for j in range(chips):
            for c in range(2):

                @pl.loop(0, last)
                def _(s):
                    put(*share(s, c, j), sem_of(s, c, j), out_recv, {"section": s, "tensor": z * 2 + c})

                @pl.when(core == c)
                def _():
                    pltpu.make_async_copy(*share(last, c, j), out_recv).start()

                @pl.when(core != c)
                def _():
                    put(*share(last, c, j), sem_of(last, c, j), out_recv, sibling)

        for j in range(chips):
            for c in range(2):

                @pl.loop(0, last)
                def _(s):
                    wait_for(stream.at[0, pl.ds(0, row_dev)], sem_of(s, c, j))

                @pl.when(core != c)
                def _():
                    wait_for(stream.at[0, pl.ds(0, row_dev)], sem_of(last, c, j))

    @pl.when(sec == 0)
    def _():
        for k, (s, d) in enumerate(near):
            if d:
                wait_for(first, i_send.at[k])

    others = pl.ds(0, rows - row_dev)
    wait_for(qkv_out.at[:, others], a2a_send)
    for copy in pushes + x_sent + m_sent:
        copy.wait_send()
    wait_for(out_ref, out_recv)


def solution(mesh):
    nc, nsec = mesh.shape["tensor"] // 2, mesh.shape["section"]

    def step(hidden, norm_gain, query_weight, query_bias, kv_weight, out_weight, kv_pool, page_table, context_len):
        all_rows, width = hidden.shape
        features, hd = query_weight.shape[1:]
        pages, page_len, kv_width = kv_pool.shape[1:]
        row_dev, blocks = page_table.shape
        part = 2 * kv_weight.shape[2]
        kvh = kv_width // (2 * hd)
        cached = row_dev * kvh * blocks * page_len
        heads = 2 * nc
        rows = all_rows // 2
        q_rows = rows * heads // nc
        anywhere = pl.BlockSpec(memory_space=pl.ANY)
        scalars = pl.BlockSpec(memory_space=pltpu.SMEM)
        dma = pltpu.SemaphoreType.DMA
        vmem = pltpu.VMEM
        return pl.pallas_call(
            functools.partial(kernel, nc, nsec),
            out_shape=jax.ShapeDtypeStruct((all_rows // nsec, width), BF16),
            in_specs=[anywhere] * 7 + [scalars] * 2,
            out_specs=pl.BlockSpec(memory_space=vmem),
            scratch_shapes=[
                vmem((2, all_rows, width), BF16),
                vmem((1, features), BF16),
                vmem((2 * nc, 1, width), F32),
                vmem((features, 2 * hd), BF16),
                vmem((2, 1, hd), BF16),
                vmem((part, features), BF16),
                vmem((heads * hd, 2 * width), BF16),
                vmem((pages, page_len, kv_width), BF16),
                vmem((cached, hd), BF16),
                vmem((cached, hd), BF16),
                vmem((q_rows, hd), F32),
                vmem((q_rows, hd), F32),
                vmem((q_rows, hd), F32),
                vmem((2, rows, width), BF16),
                vmem((nc, 2, rows, width), BF16),
                vmem((3, rows, hd), BF16),
                vmem((3, rows, hd), BF16),
                vmem((heads, row_dev, hd), BF16),
                vmem((heads, nc, row_dev, hd), BF16),
                vmem((2, rows, width), BF16),
                dma((7,)),
                dma((5,)),
                dma((5,)),
                dma((2 * nc,)),
                dma((nc,)),
                dma((nc,)),
                dma((nc,)),
                dma,
                dma,
                dma((2 * nc,)),
                dma((2 * nc,)),
                dma((nc,)),
                dma((2 * nc,)),
                dma,
                pltpu.SemaphoreType.REGULAR,
                pltpu.SemaphoreType.REGULAR,
            ],
            compiler_params=pltpu.CompilerParams(collective_id=0, has_side_effects=True),
        )(
            hidden,
            norm_gain,
            query_weight[0],
            query_bias,
            kv_weight[0].T,
            out_weight[0],
            kv_pool[0],
            page_table,
            context_len,
        )

    tensor = "tensor"
    return jax.shard_map(
        step,
        mesh=mesh,
        in_specs=(
            P("groups", tensor),
            P("section", None),
            P("section", None, tensor),
            P("section", tensor),
            P("section", None, tensor),
            P("section", None, tensor),
            P("section", ("groups", tensor), None, None),
            P(("groups", tensor), None),
            P(("groups", tensor)),
        ),
        out_specs=P(("groups", "section"), tensor),
        check_vma=False,
    )
```

```python
import functools

import jax
import jax.numpy as jnp
from jax import lax
from jax.experimental import pallas as pl
from jax.experimental.pallas import tpu as pltpu
from jax.sharding import PartitionSpec as P

MESH = pl.DeviceIdType.MESH
EPSILON = 1e-06
LOG_ROPE_BASE = 13.815510557964274
BF16 = jnp.bfloat16
F32 = jnp.float32


def relay_tree(half):
    far = half // 2
    return {d: 0 if d <= far else far for d in range(1, half + 1)}


def kernel(
    nc,
    nsec,
    hidden_hbm,
    gain_hbm,
    wq_hbm,
    bias_hbm,
    wkv_hbm,
    wo_hbm,
    pool_hbm,
    table_ref,
    len_ref,
    out_ref,
    hid,
    gain_in,
    gain,
    wq,
    bias,
    wkv,
    wo,
    pool,
    keys,
    values,
    cos_tab,
    sin_tab,
    lim_tab,
    first,
    xbuf,
    qkv_out,
    qkv_in,
    mix_own,
    mixbuf,
    stream,
    load_sems,
    push_send,
    push_recv,
    x_send,
    x_recv,
    i_send,
    r_send,
    a2a_send,
    a2a_recv,
    m_send,
    m_root,
    m_recv,
    out_send,
    out_recv,
    ready,
    turn,
):
    row_dev, blocks = table_ref.shape
    width = hid.shape[2]
    rows = nc * row_dev
    hd = keys.shape[2]
    heads = mix_own.shape[0]
    page_len = pool.shape[1]
    span = page_len * blocks
    wide = keys.shape[1]
    kvh = wide // row_dev // span
    per_chip = heads // nc
    part = wkv.shape[0]
    half = nc // 2
    parent = relay_tree(half)
    kids = {d: sorted((c for c in parent if parent[c] == d), reverse=True) for d in range(half + 1)}
    far = half // 2
    near = [(s, d) for d in range(far, 0, -1) for s in (1, -1)] + [(1, 0)]

    me = lax.axis_index("tensor")
    sec = lax.axis_index("section")
    z = me // 2
    core = lax.rem(me, 2)
    last = nsec - 1
    turnover = nsec // 2
    flip = sec // turnover
    piece = lax.rem(core + flip, 2)

    def dev(zz, s=None):
        where = {"tensor": lax.rem(zz + 2 * nc, nc) * 2 + core}
        if s is not None:
            where["section"] = s
        return where

    def ahead(zz):
        other = lax.rem(core + (sec + 1) // turnover + flip, 2)
        return {"tensor": lax.rem(zz + 2 * nc, nc) * 2 + other, "section": sec + 1}

    def behind(zz):
        other = lax.rem(core + (sec - 1) // turnover + flip, 2)
        return {"tensor": lax.rem(zz + 2 * nc, nc) * 2 + other, "section": sec - 1}

    def put(src, dst, ssem, rsem, where):
        copy = pltpu.make_async_remote_copy(
            src_ref=src, dst_ref=dst, send_sem=ssem, recv_sem=rsem, device_id=where, device_id_type=MESH
        )
        copy.start()
        return copy

    def wait_for(ref, sem):
        pltpu.make_async_copy(ref, ref, sem).wait()

    def cut(ref, axis, c):
        n = ref.shape[axis] // 2
        at = pl.multiple_of(c * n, n)
        return ref.at[pl.ds(at, n)] if axis == 0 else ref.at[:, pl.ds(at, n)]

    def shares(c):
        return [hid.at[c], bias.at[c], cut(wq, 1, c), cut(wkv, 0, c), cut(wo, 1, c)]

    sources = [hidden_hbm, bias_hbm, wq_hbm, wkv_hbm, wo_hbm]

    def load(k, src, dst):
        copy = pltpu.make_async_copy(src, dst, load_sems.at[k])
        copy.start()
        return copy

    load_gain, load_pool = load(0, gain_hbm, gain_in), load(1, pool_hbm, pool)
    own_loads = [load(2 + k, src, dst) for k, (src, dst) in enumerate(zip(sources, shares(core)))]

    barrier = pltpu.get_barrier_semaphore()

    def greet(where):
        pl.semaphore_signal(barrier, inc=1, device_id=where, device_id_type=MESH)

    sibling = {"tensor": z * 2 + 1 - core}
    greet(sibling)

    @pl.loop(1, nc)
    def _(i):
        greet(dev(z + i))

    @pl.when(sec < last)
    def _():
        for s, d in near:
            greet(ahead(z + s * d))

    @pl.when(sec > 0)
    def _():
        pl.semaphore_wait(barrier, nc + len(near))
        for s, d in near:
            pl.semaphore_signal(ready, inc=1, device_id=behind(z - s * d), device_id_type=MESH)

    @pl.when(sec == 0)
    def _():
        pl.semaphore_wait(barrier, nc)

    pushes = [
        put(src, dst, push_send.at[k], push_recv.at[k], sibling)
        for k, (src, dst) in enumerate(zip(sources, shares(core)))
    ]

    def send_stream(src, sems):
        return [put(src, xbuf.at[z], sems.at[k], x_recv.at[z], ahead(z + s * d)) for k, (s, d) in enumerate(near)]

    own_loads[0].wait()
    wait_for(hid.at[0], push_recv.at[0])

    @pl.when(jnp.logical_and(sec == 0, core == 1))
    def _():
        pl.semaphore_wait(turn, 1)

    @pl.when(sec == 0)
    def _():
        whole = 2 * rows
        at = lax.broadcasted_iota(jnp.int32, (rows, whole), 0)
        col = lax.broadcasted_iota(jnp.int32, (rows, whole), 1)
        row = (at // row_dev * 2 + core) * row_dev + lax.rem(at, row_dev)
        pick = jnp.where(col == row, 1.0, 0.0).astype(BF16)
        for c in range(2):
            first[c] = jnp.dot(pick, hid[c], preferred_element_type=F32).astype(BF16)
        for k, (s, d) in enumerate(near):
            if d:
                put(first, xbuf.at[z], i_send.at[k], x_recv.at[z], dev(z + s * d))
            else:
                pltpu.make_async_copy(first, xbuf.at[z], x_recv.at[z]).start()

    load_gain.wait()
    for t in range(2 * nc):
        gain[t] = gain_in[:, t * width : (t + 1) * width].astype(F32)
    load_pool.wait()
    for r in range(row_dev):
        for b in range(blocks):
            page = pool[lax.rem(table_ref[r, b], pool.shape[0])]
            for k in range(kvh):
                at = (r * kvh + k) * span + b * page_len
                keys[0, at : at + page_len, :] = page[:, k * hd : (k + 1) * hd]
                values[0, at : at + page_len, :] = page[:, (kvh + k) * hd : (kvh + k + 1) * hd]

    q_rows = per_chip * rows
    lane = lax.broadcasted_iota(jnp.int32, (q_rows, hd), 1)
    sample = lax.rem(lax.broadcasted_iota(jnp.int32, (q_rows, hd), 0), row_dev)
    position = jnp.full((q_rows, hd), len_ref[0], jnp.int32)
    for r in range(1, row_dev):
        position = jnp.where(sample == r, len_ref[r], position)
    position = position.astype(F32)
    frequency = jnp.exp(lax.rem(lane, hd // 2).astype(F32) * (-2.0 * LOG_ROPE_BASE / hd))
    angle = position * frequency
    sine = jnp.sin(angle)
    cos_tab[0] = jnp.cos(angle)
    sin_tab[0] = jnp.where(lane < hd // 2, -sine, sine)
    lim_tab[0] = position
    tables = [keys, values, cos_tab, sin_tab, lim_tab]

    @pl.when(flip == 1)
    def _():
        for k, table in enumerate(tables):
            put(table.at[0], table.at[1], push_send.at[len(sources) + k], push_recv.at[len(sources) + k], sibling)

    for k in range(1, 4):
        own_loads[k].wait()
        wait_for(shares(0)[k], push_recv.at[k])

    def chip_at(d, s):
        return lax.rem(z - s * d + nc, nc)

    def in_half(ref, s):
        n = ref.shape[0] // 2
        return ref.at[pl.ds(0 if s == 1 else n, n)]

    ring = [(far, 1), (far, -1)]
    ring += [(d, s) for d in range(1, half) if d != far for s in (1, -1)] + [(half, 1)]

    def pass_turn():
        @pl.when(jnp.logical_and(sec == 0, core == 0))
        def _():
            pl.semaphore_signal(turn, inc=1, device_id=sibling, device_id_type=MESH)

    def relay(place, recv, sems, items, direct, use, after_far=None):
        sent, passed = [], []
        for d, s in items:
            chip = chip_at(d, s)
            block = place(chip)
            wait_for(block, recv.at[chip])
            if d != far and passed:
                if after_far:
                    after_far()
                    after_far = None
                use(passed)
                passed = []
            passed.append(chip)
            for c in kids[d] if (d, s) not in direct else []:
                piece = in_half(block, s) if c == half else block
                sent.append(put(piece, piece, sems.at[len(sent)], recv.at[chip], dev(z + s * (c - d))))
        use(passed)
        return sent

    sums = {
        "q": jnp.zeros((rows, per_chip * hd), F32),
        "kv": jnp.zeros((rows, part), F32),
        "squares": jnp.zeros((rows, width), F32),
    }

    def project(chips):
        for chip in chips:
            project_one(chip)

    def project_one(chip):
        parts = []
        for c in range(2):
            x = xbuf[chip, c].astype(F32)
            sums["squares"] += x * x
            parts.append((x * gain[chip * 2 + c]).astype(BF16))
        y = jnp.concatenate(parts, axis=1)
        at = pl.multiple_of(chip * 2 * width, 2 * width)
        sums["q"] += jnp.dot(y, wq[pl.ds(at, 2 * width), :], preferred_element_type=F32)
        sums["kv"] += lax.dot_general(
            y, wkv[:, pl.ds(at, 2 * width)], (((1,), (1,)), ((), ())), preferred_element_type=F32
        )

    x_sent = relay(
        lambda c: xbuf.at[c], x_recv, x_send, ring[:2] + [(0, 1)] + ring[2:], [(0, 1)], project
    )

    def mine(ref, c):
        return ref.at[:, pl.ds(c * row_dev, row_dev)]

    scale = lax.rsqrt(jnp.sum(sums["squares"], axis=1, keepdims=True) / (2 * nc * width) + EPSILON)
    for i in range(per_chip):
        q = sums["q"][:, i * hd : (i + 1) * hd] * scale + bias[i].astype(F32)
        qkv_out[i] = q.astype(BF16)
    kv = (sums["kv"] * scale).astype(BF16).astype(F32)
    kv = jnp.concatenate([kv, jnp.zeros((rows, hd - part), F32)], axis=1)
    kv = pltpu.roll(kv, lax.rem(z, hd // part) * part, 1)
    qkv_out[per_chip] = kv.astype(BF16)

    for i in range(nc - 1):
        c = lax.rem(z + half + (1 - 2 * (i % 2)) * ((i + 1) // 2) + nc, nc)
        put(mine(qkv_out, c), mine(qkv_in, z), a2a_send, a2a_recv, dev(c))

    pltpu.make_async_copy(mine(qkv_out, z), mine(qkv_in, z), a2a_recv).start()
    pass_turn()

    @pl.when(flip == 1)
    def _():
        for k, table in enumerate(tables):
            wait_for(table.at[1], push_recv.at[len(sources) + k])

    def grid(shape, axis):
        return lax.broadcasted_iota(jnp.int32, shape, axis)

    group = heads // kvh
    q_of, c_of = grid((q_rows, wide), 0), grid((q_rows, wide), 1)
    key_head = (lax.rem(q_of, rows) // row_dev * per_chip + q_of // rows) // group
    matching = c_of // span == lax.rem(q_of, row_dev) * kvh + key_head
    usable = matching & (lax.rem(c_of, span).astype(F32) < lim_tab[flip][:, :1])
    s_row, s_col = grid((q_rows, rows), 0), grid((q_rows, rows), 1)
    same = lax.rem(s_row, row_dev) == lax.rem(s_col, row_dev)
    source = s_col // row_dev // (hd // part)
    wanted = (lax.rem(s_row, rows) // row_dev * per_chip + s_row // rows) // group
    pick_key = jnp.where(same & (source == wanted), 1.0, 0.0).astype(BF16)
    pick_value = jnp.where(same & (source == wanted + kvh), 1.0, 0.0).astype(BF16)
    root = hd ** (-0.5)
    cos, sin = cos_tab[flip], sin_tab[flip]
    wait_for(qkv_in, a2a_recv)

    def rotate(v):
        return (v * cos + pltpu.roll(v, hd // 2, 1) * sin).astype(BF16)

    rotated = rotate(jnp.concatenate([qkv_in[i].astype(F32) for i in range(per_chip)], axis=0))
    fresh = qkv_in[per_chip]
    key_new = rotate(jnp.dot(pick_key, fresh, preferred_element_type=F32))
    value_new = jnp.dot(pick_value, fresh, preferred_element_type=F32)
    scores = lax.dot_general(rotated, keys[flip], (((1,), (1,)), ((), ())), preferred_element_type=F32) * root
    own_score = jnp.sum(rotated.astype(F32) * key_new.astype(F32), axis=1, keepdims=True) * root
    top = jnp.maximum(jnp.max(jnp.where(usable, scores, -1e30), axis=1, keepdims=True), own_score)
    weights = jnp.where(usable, jnp.exp(scores - top), 0.0)
    own_weight = jnp.exp(own_score - top)
    total = jnp.sum(weights, axis=1, keepdims=True) + own_weight
    weights = (weights / total).astype(BF16)
    own_weight = (own_weight / total).astype(BF16).astype(F32)
    mixture = jnp.dot(weights, values[flip], preferred_element_type=F32) + own_weight * value_new
    mix_own[...] = mixture.astype(BF16).reshape(heads, row_dev, hd)

    def mix_place(c):
        return mixbuf.at[:, c]

    m_sent = []
    for c in kids[0]:
        for s in (1, -1):
            m_sent.append(put(mix_own, mix_place(z), m_root.at[len(m_sent)], m_recv.at[z], dev(z + s * c)))
    pltpu.make_async_copy(mix_own, mix_place(z), m_recv.at[z]).start()
    m_sent += relay(mix_place, m_recv, m_send, ring, [], lambda chips: None)
    wait_for(mix_place(z), m_recv.at[z])

    own_loads[4].wait()
    wait_for(shares(0)[4], push_recv.at[4])

    mixed = [mixbuf[i * nc + c].reshape(rows, hd) for c in range(nc) for i in range(per_chip)]
    change = jnp.dot(jnp.concatenate(mixed, axis=1), wo[...], preferred_element_type=F32)
    for c in range(2):
        x = xbuf[z, c].astype(F32)
        stream[c] = (x + change[:, c * width : (c + 1) * width]).astype(BF16)

    chips = nc // nsec

    @pl.when(sec < last)
    def _():
        pl.semaphore_wait(ready, len(near))
        for copy in send_stream(stream, r_send):
            copy.wait_send()

    @pl.when(sec == last)
    def _():
        def share(s, c, j):
            return (
                stream.at[c, pl.ds((s * chips + j) * row_dev, row_dev)],
                out_ref.at[pl.ds((j * 2 + piece) * row_dev, row_dev)],
            )

        def sem_of(s, c, j):
            return out_send.at[(j * 2 + c) * nsec + s]

        for j in range(chips):
            for c in range(2):

                @pl.loop(0, last)
                def _(s):
                    put(*share(s, c, j), sem_of(s, c, j), out_recv, {"section": s, "tensor": z * 2 + c})

                @pl.when(core == c)
                def _():
                    pltpu.make_async_copy(*share(last, c, j), out_recv).start()

                @pl.when(core != c)
                def _():
                    put(*share(last, c, j), sem_of(last, c, j), out_recv, sibling)

        for j in range(chips):
            for c in range(2):

                @pl.loop(0, last)
                def _(s):
                    wait_for(stream.at[0, pl.ds(0, row_dev)], sem_of(s, c, j))

                @pl.when(core != c)
                def _():
                    wait_for(stream.at[0, pl.ds(0, row_dev)], sem_of(last, c, j))

    @pl.when(sec == 0)
    def _():
        for k, (s, d) in enumerate(near):
            if d:
                wait_for(first, i_send.at[k])

    @pl.when(flip == 1)
    def _():
        for k, table in enumerate(tables):
            wait_for(table.at[0], push_send.at[len(sources) + k])

    others = pl.ds(0, rows - row_dev)
    wait_for(qkv_out.at[:, others], a2a_send)
    for copy in pushes + x_sent + m_sent:
        copy.wait_send()
    wait_for(out_ref, out_recv)


def solution(mesh):
    nc, nsec = mesh.shape["tensor"] // 2, mesh.shape["section"]

    def step(hidden, norm_gain, query_weight, query_bias, kv_weight, out_weight, kv_pool, page_table, context_len):
        all_rows, width = hidden.shape
        features, hd = query_weight.shape[1:]
        pages, page_len, kv_width = kv_pool.shape[1:]
        row_dev, blocks = page_table.shape
        part = 2 * kv_weight.shape[2]
        kvh = kv_width // (2 * hd)
        cached = row_dev * kvh * blocks * page_len
        heads = 2 * nc
        rows = all_rows // 2
        q_rows = rows * heads // nc
        anywhere = pl.BlockSpec(memory_space=pl.ANY)
        scalars = pl.BlockSpec(memory_space=pltpu.SMEM)
        dma = pltpu.SemaphoreType.DMA
        vmem = pltpu.VMEM
        return pl.pallas_call(
            functools.partial(kernel, nc, nsec),
            out_shape=jax.ShapeDtypeStruct((all_rows // nsec, width), BF16),
            in_specs=[anywhere] * 7 + [scalars] * 2,
            out_specs=pl.BlockSpec(memory_space=vmem),
            scratch_shapes=[
                vmem((2, all_rows, width), BF16),
                vmem((1, features), BF16),
                vmem((2 * nc, 1, width), F32),
                vmem((features, 2 * hd), BF16),
                vmem((2, 1, hd), BF16),
                vmem((part, features), BF16),
                vmem((heads * hd, 2 * width), BF16),
                vmem((pages, page_len, kv_width), BF16),
                vmem((2, cached, hd), BF16),
                vmem((2, cached, hd), BF16),
                vmem((2, q_rows, hd), F32),
                vmem((2, q_rows, hd), F32),
                vmem((2, q_rows, hd), F32),
                vmem((2, rows, width), BF16),
                vmem((nc, 2, rows, width), BF16),
                vmem((3, rows, hd), BF16),
                vmem((3, rows, hd), BF16),
                vmem((heads, row_dev, hd), BF16),
                vmem((heads, nc, row_dev, hd), BF16),
                vmem((2, rows, width), BF16),
                dma((7,)),
                dma((10,)),
                dma((10,)),
                dma((2 * nc,)),
                dma((nc,)),
                dma((nc,)),
                dma((nc,)),
                dma,
                dma,
                dma((2 * nc,)),
                dma((2 * nc,)),
                dma((nc,)),
                dma((2 * nc,)),
                dma,
                pltpu.SemaphoreType.REGULAR,
                pltpu.SemaphoreType.REGULAR,
            ],
            compiler_params=pltpu.CompilerParams(collective_id=0, has_side_effects=True),
        )(
            hidden,
            norm_gain,
            query_weight[0],
            query_bias,
            kv_weight[0].T,
            out_weight[0],
            kv_pool[0],
            page_table,
            context_len,
        )

    tensor = "tensor"
    return jax.shard_map(
        step,
        mesh=mesh,
        in_specs=(
            P("groups", tensor),
            P("section", None),
            P("section", None, tensor),
            P("section", tensor),
            P("section", None, tensor),
            P("section", None, tensor),
            P("section", ("groups", tensor), None, None),
            P(("groups", tensor), None),
            P(("groups", tensor)),
        ),
        out_specs=P(("groups", "section"), tensor),
        check_vma=False,
    )
```

```python
import functools

import jax
import jax.numpy as jnp
from jax import lax
from jax.experimental import pallas as pl
from jax.experimental.pallas import tpu as pltpu
from jax.sharding import PartitionSpec as P

MESH = pl.DeviceIdType.MESH
EPSILON = 1e-06
LOG_ROPE_BASE = 13.815510557964274
BF16 = jnp.bfloat16
F32 = jnp.float32


def relay_tree(half):
    far = half // 2
    return {d: 0 if d <= far else far for d in range(1, half + 1)}


def kernel(
    nc,
    nsec,
    hidden_hbm,
    gain_hbm,
    wq_hbm,
    bias_hbm,
    wkv_hbm,
    wo_hbm,
    pool_hbm,
    table_ref,
    len_ref,
    out_ref,
    hid,
    gain_in,
    gain,
    wq,
    bias,
    wkv,
    wo,
    pool,
    keys,
    values,
    cos_tab,
    sin_tab,
    lim_tab,
    first,
    xbuf,
    qkv_out,
    qkv_in,
    mix_own,
    mixbuf,
    stream,
    load_sems,
    push_send,
    push_recv,
    x_send,
    x_recv,
    i_send,
    r_send,
    a2a_send,
    a2a_recv,
    m_send,
    m_root,
    m_recv,
    out_send,
    out_recv,
    ready,
    turn,
):
    row_dev, blocks = table_ref.shape
    width = hid.shape[2]
    rows = nc * row_dev
    hd = keys.shape[2]
    heads = mix_own.shape[0]
    page_len = pool.shape[1]
    span = page_len * blocks
    wide = keys.shape[1]
    kvh = wide // row_dev // span
    per_chip = heads // nc
    part = wkv.shape[0]
    half = nc // 2
    parent = relay_tree(half)
    kids = {d: sorted((c for c in parent if parent[c] == d), reverse=True) for d in range(half + 1)}
    far = half // 2
    near = [(s, d) for d in range(far, 0, -1) for s in (1, -1)] + [(1, 0)]

    me = lax.axis_index("tensor")
    sec = lax.axis_index("section")
    z = me // 2
    core = lax.rem(me, 2)
    last = nsec - 1
    flip = lax.rem(sec, 2)
    piece = lax.rem(core + flip, 2)

    def dev(zz, s=None):
        where = {"tensor": lax.rem(zz + 2 * nc, nc) * 2 + core}
        if s is not None:
            where["section"] = s
        return where

    def ahead(zz):
        return {"tensor": lax.rem(zz + 2 * nc, nc) * 2 + 1 - core, "section": sec + 1}

    def behind(zz):
        return {"tensor": lax.rem(zz + 2 * nc, nc) * 2 + 1 - core, "section": sec - 1}

    def put(src, dst, ssem, rsem, where):
        copy = pltpu.make_async_remote_copy(
            src_ref=src, dst_ref=dst, send_sem=ssem, recv_sem=rsem, device_id=where, device_id_type=MESH
        )
        copy.start()
        return copy

    def wait_for(ref, sem):
        pltpu.make_async_copy(ref, ref, sem).wait()

    def cut(ref, axis, c):
        n = ref.shape[axis] // 2
        at = pl.multiple_of(c * n, n)
        return ref.at[pl.ds(at, n)] if axis == 0 else ref.at[:, pl.ds(at, n)]

    def shares(c):
        return [hid.at[c], bias.at[c], cut(wq, 1, c), cut(wkv, 0, c), cut(wo, 1, c)]

    sources = [hidden_hbm, bias_hbm, wq_hbm, wkv_hbm, wo_hbm]

    def load(k, src, dst):
        copy = pltpu.make_async_copy(src, dst, load_sems.at[k])
        copy.start()
        return copy

    load_gain, load_pool = load(0, gain_hbm, gain_in), load(1, pool_hbm, pool)
    own_loads = [load(2 + k, src, dst) for k, (src, dst) in enumerate(zip(sources, shares(core)))]

    barrier = pltpu.get_barrier_semaphore()

    def greet(where):
        pl.semaphore_signal(barrier, inc=1, device_id=where, device_id_type=MESH)

    sibling = {"tensor": z * 2 + 1 - core}
    greet(sibling)

    @pl.loop(1, nc)
    def _(i):
        greet(dev(z + i))

    @pl.when(sec < last)
    def _():
        for s, d in near:
            greet(ahead(z + s * d))

    @pl.when(sec > 0)
    def _():
        pl.semaphore_wait(barrier, nc + len(near))
        for s, d in near:
            pl.semaphore_signal(ready, inc=1, device_id=behind(z - s * d), device_id_type=MESH)

    @pl.when(sec == 0)
    def _():
        pl.semaphore_wait(barrier, nc)

    pushes = [
        put(src, dst, push_send.at[k], push_recv.at[k], sibling)
        for k, (src, dst) in enumerate(zip(sources, shares(core)))
    ]

    def send_stream(src, sems):
        return [put(src, xbuf.at[z], sems.at[k], x_recv.at[z], ahead(z + s * d)) for k, (s, d) in enumerate(near)]

    own_loads[0].wait()
    wait_for(hid.at[0], push_recv.at[0])

    @pl.when(jnp.logical_and(sec == 0, core == 1))
    def _():
        pl.semaphore_wait(turn, 1)

    @pl.when(sec == 0)
    def _():
        whole = 2 * rows
        at = lax.broadcasted_iota(jnp.int32, (rows, whole), 0)
        col = lax.broadcasted_iota(jnp.int32, (rows, whole), 1)
        row = (at // row_dev * 2 + core) * row_dev + lax.rem(at, row_dev)
        pick = jnp.where(col == row, 1.0, 0.0).astype(BF16)
        for c in range(2):
            first[c] = jnp.dot(pick, hid[c], preferred_element_type=F32).astype(BF16)
        for k, (s, d) in enumerate(near):
            if d:
                put(first, xbuf.at[z], i_send.at[k], x_recv.at[z], dev(z + s * d))
            else:
                pltpu.make_async_copy(first, xbuf.at[z], x_recv.at[z]).start()

    load_gain.wait()
    for t in range(2 * nc):
        gain[t] = gain_in[:, t * width : (t + 1) * width].astype(F32)
    load_pool.wait()
    for r in range(row_dev):
        for b in range(blocks):
            page = pool[lax.rem(table_ref[r, b], pool.shape[0])]
            for k in range(kvh):
                at = (r * kvh + k) * span + b * page_len
                keys[0, at : at + page_len, :] = page[:, k * hd : (k + 1) * hd]
                values[0, at : at + page_len, :] = page[:, (kvh + k) * hd : (kvh + k + 1) * hd]

    q_rows = per_chip * rows
    lane = lax.broadcasted_iota(jnp.int32, (q_rows, hd), 1)
    sample = lax.rem(lax.broadcasted_iota(jnp.int32, (q_rows, hd), 0), row_dev)
    position = jnp.full((q_rows, hd), len_ref[0], jnp.int32)
    for r in range(1, row_dev):
        position = jnp.where(sample == r, len_ref[r], position)
    position = position.astype(F32)
    frequency = jnp.exp(lax.rem(lane, hd // 2).astype(F32) * (-2.0 * LOG_ROPE_BASE / hd))
    angle = position * frequency
    sine = jnp.sin(angle)
    cos_tab[0] = jnp.cos(angle)
    sin_tab[0] = jnp.where(lane < hd // 2, -sine, sine)
    lim_tab[0] = position
    tables = [keys, values, cos_tab, sin_tab, lim_tab]

    @pl.when(flip == 1)
    def _():
        for k, table in enumerate(tables):
            put(table.at[0], table.at[1], push_send.at[len(sources) + k], push_recv.at[len(sources) + k], sibling)

    for k in range(1, 4):
        own_loads[k].wait()
        wait_for(shares(0)[k], push_recv.at[k])

    def chip_at(d, s):
        return lax.rem(z - s * d + nc, nc)

    def in_half(ref, s):
        n = ref.shape[0] // 2
        return ref.at[pl.ds(0 if s == 1 else n, n)]

    ring = [(far, 1), (far, -1)]
    ring += [(d, s) for d in range(1, half) if d != far for s in (1, -1)] + [(half, 1)]

    def pass_turn():
        @pl.when(jnp.logical_and(sec == 0, core == 0))
        def _():
            pl.semaphore_signal(turn, inc=1, device_id=sibling, device_id_type=MESH)

    def relay(place, recv, sems, items, direct, use, after_far=None):
        sent, passed = [], []
        for d, s in items:
            chip = chip_at(d, s)
            block = place(chip)
            wait_for(block, recv.at[chip])
            if d != far and passed:
                if after_far:
                    after_far()
                    after_far = None
                use(passed)
                passed = []
            passed.append(chip)
            for c in kids[d] if (d, s) not in direct else []:
                piece = in_half(block, s) if c == half else block
                sent.append(put(piece, piece, sems.at[len(sent)], recv.at[chip], dev(z + s * (c - d))))
        use(passed)
        return sent

    sums = {
        "q": jnp.zeros((rows, per_chip * hd), F32),
        "kv": jnp.zeros((rows, part), F32),
        "squares": jnp.zeros((rows, width), F32),
    }

    def project(chips):
        for chip in chips:
            project_one(chip)

    def project_one(chip):
        parts = []
        for c in range(2):
            x = xbuf[chip, c].astype(F32)
            sums["squares"] += x * x
            parts.append((x * gain[chip * 2 + c]).astype(BF16))
        y = jnp.concatenate(parts, axis=1)
        at = pl.multiple_of(chip * 2 * width, 2 * width)
        sums["q"] += jnp.dot(y, wq[pl.ds(at, 2 * width), :], preferred_element_type=F32)
        sums["kv"] += lax.dot_general(
            y, wkv[:, pl.ds(at, 2 * width)], (((1,), (1,)), ((), ())), preferred_element_type=F32
        )

    x_sent = relay(
        lambda c: xbuf.at[c], x_recv, x_send, ring[:2] + [(0, 1)] + ring[2:], [(0, 1)], project
    )

    def mine(ref, c):
        return ref.at[:, pl.ds(c * row_dev, row_dev)]

    scale = lax.rsqrt(jnp.sum(sums["squares"], axis=1, keepdims=True) / (2 * nc * width) + EPSILON)
    for i in range(per_chip):
        q = sums["q"][:, i * hd : (i + 1) * hd] * scale + bias[i].astype(F32)
        qkv_out[i] = q.astype(BF16)
    kv = (sums["kv"] * scale).astype(BF16).astype(F32)
    kv = jnp.concatenate([kv, jnp.zeros((rows, hd - part), F32)], axis=1)
    kv = pltpu.roll(kv, lax.rem(z, hd // part) * part, 1)
    qkv_out[per_chip] = kv.astype(BF16)

    for i in range(nc - 1):
        c = lax.rem(z + half + (1 - 2 * (i % 2)) * ((i + 1) // 2) + nc, nc)
        put(mine(qkv_out, c), mine(qkv_in, z), a2a_send, a2a_recv, dev(c))

    pltpu.make_async_copy(mine(qkv_out, z), mine(qkv_in, z), a2a_recv).start()
    pass_turn()

    @pl.when(flip == 1)
    def _():
        for k, table in enumerate(tables):
            wait_for(table.at[1], push_recv.at[len(sources) + k])

    def grid(shape, axis):
        return lax.broadcasted_iota(jnp.int32, shape, axis)

    group = heads // kvh
    q_of, c_of = grid((q_rows, wide), 0), grid((q_rows, wide), 1)
    key_head = (lax.rem(q_of, rows) // row_dev * per_chip + q_of // rows) // group
    matching = c_of // span == lax.rem(q_of, row_dev) * kvh + key_head
    usable = matching & (lax.rem(c_of, span).astype(F32) < lim_tab[flip][:, :1])
    s_row, s_col = grid((q_rows, rows), 0), grid((q_rows, rows), 1)
    same = lax.rem(s_row, row_dev) == lax.rem(s_col, row_dev)
    source = s_col // row_dev // (hd // part)
    wanted = (lax.rem(s_row, rows) // row_dev * per_chip + s_row // rows) // group
    pick_key = jnp.where(same & (source == wanted), 1.0, 0.0).astype(BF16)
    pick_value = jnp.where(same & (source == wanted + kvh), 1.0, 0.0).astype(BF16)
    root = hd ** (-0.5)
    cos, sin = cos_tab[flip], sin_tab[flip]
    wait_for(qkv_in, a2a_recv)

    def rotate(v):
        return (v * cos + pltpu.roll(v, hd // 2, 1) * sin).astype(BF16)

    rotated = rotate(jnp.concatenate([qkv_in[i].astype(F32) for i in range(per_chip)], axis=0))
    fresh = qkv_in[per_chip]
    key_new = rotate(jnp.dot(pick_key, fresh, preferred_element_type=F32))
    value_new = jnp.dot(pick_value, fresh, preferred_element_type=F32)
    scores = lax.dot_general(rotated, keys[flip], (((1,), (1,)), ((), ())), preferred_element_type=F32) * root
    own_score = jnp.sum(rotated.astype(F32) * key_new.astype(F32), axis=1, keepdims=True) * root
    top = jnp.maximum(jnp.max(jnp.where(usable, scores, -1e30), axis=1, keepdims=True), own_score)
    weights = jnp.where(usable, jnp.exp(scores - top), 0.0)
    own_weight = jnp.exp(own_score - top)
    total = jnp.sum(weights, axis=1, keepdims=True) + own_weight
    weights = (weights / total).astype(BF16)
    own_weight = (own_weight / total).astype(BF16).astype(F32)
    mixture = jnp.dot(weights, values[flip], preferred_element_type=F32) + own_weight * value_new
    mix_own[...] = mixture.astype(BF16).reshape(heads, row_dev, hd)

    def mix_place(c):
        return mixbuf.at[:, c]

    m_sent = []
    for c in kids[0]:
        for s in (1, -1):
            m_sent.append(put(mix_own, mix_place(z), m_root.at[len(m_sent)], m_recv.at[z], dev(z + s * c)))
    pltpu.make_async_copy(mix_own, mix_place(z), m_recv.at[z]).start()
    m_sent += relay(mix_place, m_recv, m_send, ring, [], lambda chips: None)
    wait_for(mix_place(z), m_recv.at[z])

    own_loads[4].wait()
    wait_for(shares(0)[4], push_recv.at[4])

    mixed = [mixbuf[i * nc + c].reshape(rows, hd) for c in range(nc) for i in range(per_chip)]
    change = jnp.dot(jnp.concatenate(mixed, axis=1), wo[...], preferred_element_type=F32)
    for c in range(2):
        x = xbuf[z, c].astype(F32)
        stream[c] = (x + change[:, c * width : (c + 1) * width]).astype(BF16)

    chips = nc // nsec

    @pl.when(sec < last)
    def _():
        pl.semaphore_wait(ready, len(near))
        for copy in send_stream(stream, r_send):
            copy.wait_send()

    @pl.when(sec == last)
    def _():
        def share(s, c, j):
            return (
                stream.at[c, pl.ds((s * chips + j) * row_dev, row_dev)],
                out_ref.at[pl.ds((j * 2 + piece) * row_dev, row_dev)],
            )

        def sem_of(s, c, j):
            return out_send.at[(j * 2 + c) * nsec + s]

        for j in range(chips):
            for c in range(2):

                @pl.loop(0, last)
                def _(s):
                    put(*share(s, c, j), sem_of(s, c, j), out_recv, {"section": s, "tensor": z * 2 + c})

                @pl.when(core == c)
                def _():
                    pltpu.make_async_copy(*share(last, c, j), out_recv).start()

                @pl.when(core != c)
                def _():
                    put(*share(last, c, j), sem_of(last, c, j), out_recv, sibling)

        for j in range(chips):
            for c in range(2):

                @pl.loop(0, last)
                def _(s):
                    wait_for(stream.at[0, pl.ds(0, row_dev)], sem_of(s, c, j))

                @pl.when(core != c)
                def _():
                    wait_for(stream.at[0, pl.ds(0, row_dev)], sem_of(last, c, j))

    @pl.when(sec == 0)
    def _():
        for k, (s, d) in enumerate(near):
            if d:
                wait_for(first, i_send.at[k])

    @pl.when(flip == 1)
    def _():
        for k, table in enumerate(tables):
            wait_for(table.at[0], push_send.at[len(sources) + k])

    others = pl.ds(0, rows - row_dev)
    wait_for(qkv_out.at[:, others], a2a_send)
    for copy in pushes + x_sent + m_sent:
        copy.wait_send()
    wait_for(out_ref, out_recv)


def solution(mesh):
    nc, nsec = mesh.shape["tensor"] // 2, mesh.shape["section"]

    def step(hidden, norm_gain, query_weight, query_bias, kv_weight, out_weight, kv_pool, page_table, context_len):
        all_rows, width = hidden.shape
        features, hd = query_weight.shape[1:]
        pages, page_len, kv_width = kv_pool.shape[1:]
        row_dev, blocks = page_table.shape
        part = 2 * kv_weight.shape[2]
        kvh = kv_width // (2 * hd)
        cached = row_dev * kvh * blocks * page_len
        heads = 2 * nc
        rows = all_rows // 2
        q_rows = rows * heads // nc
        anywhere = pl.BlockSpec(memory_space=pl.ANY)
        scalars = pl.BlockSpec(memory_space=pltpu.SMEM)
        dma = pltpu.SemaphoreType.DMA
        vmem = pltpu.VMEM
        return pl.pallas_call(
            functools.partial(kernel, nc, nsec),
            out_shape=jax.ShapeDtypeStruct((all_rows // nsec, width), BF16),
            in_specs=[anywhere] * 7 + [scalars] * 2,
            out_specs=pl.BlockSpec(memory_space=vmem),
            scratch_shapes=[
                vmem((2, all_rows, width), BF16),
                vmem((1, features), BF16),
                vmem((2 * nc, 1, width), F32),
                vmem((features, 2 * hd), BF16),
                vmem((2, 1, hd), BF16),
                vmem((part, features), BF16),
                vmem((heads * hd, 2 * width), BF16),
                vmem((pages, page_len, kv_width), BF16),
                vmem((2, cached, hd), BF16),
                vmem((2, cached, hd), BF16),
                vmem((2, q_rows, hd), F32),
                vmem((2, q_rows, hd), F32),
                vmem((2, q_rows, hd), F32),
                vmem((2, rows, width), BF16),
                vmem((nc, 2, rows, width), BF16),
                vmem((3, rows, hd), BF16),
                vmem((3, rows, hd), BF16),
                vmem((heads, row_dev, hd), BF16),
                vmem((heads, nc, row_dev, hd), BF16),
                vmem((2, rows, width), BF16),
                dma((7,)),
                dma((10,)),
                dma((10,)),
                dma((2 * nc,)),
                dma((nc,)),
                dma((nc,)),
                dma((nc,)),
                dma,
                dma,
                dma((2 * nc,)),
                dma((2 * nc,)),
                dma((nc,)),
                dma((2 * nc,)),
                dma,
                pltpu.SemaphoreType.REGULAR,
                pltpu.SemaphoreType.REGULAR,
            ],
            compiler_params=pltpu.CompilerParams(collective_id=0, has_side_effects=True),
        )(
            hidden,
            norm_gain,
            query_weight[0],
            query_bias,
            kv_weight[0].T,
            out_weight[0],
            kv_pool[0],
            page_table,
            context_len,
        )

    tensor = "tensor"
    return jax.shard_map(
        step,
        mesh=mesh,
        in_specs=(
            P("groups", tensor),
            P("section", None),
            P("section", None, tensor),
            P("section", tensor),
            P("section", None, tensor),
            P("section", None, tensor),
            P("section", ("groups", tensor), None, None),
            P(("groups", tensor), None),
            P(("groups", tensor)),
        ),
        out_specs=P(("groups", "section"), tensor),
        check_vma=False,
    )
```

```python
import functools

import jax
import jax.numpy as jnp
from jax import lax
from jax.experimental import pallas as pl
from jax.experimental.pallas import tpu as pltpu
from jax.sharding import PartitionSpec as P

MESH = pl.DeviceIdType.MESH
EPSILON = 1e-06
LOG_ROPE_BASE = 13.815510557964274
BF16 = jnp.bfloat16
F32 = jnp.float32


def relay_tree(half):
    far = half // 2
    return {d: 0 if d <= far else far for d in range(1, half + 1)}


def kernel(
    nc,
    nsec,
    hidden_hbm,
    gain_hbm,
    wq_hbm,
    bias_hbm,
    wkv_hbm,
    wo_hbm,
    pool_hbm,
    table_ref,
    len_ref,
    out_ref,
    hid,
    gain_in,
    gain,
    wq,
    bias,
    wkv,
    wo,
    pool,
    keys,
    values,
    cos_tab,
    sin_tab,
    lim_tab,
    first,
    xbuf,
    qkv_out,
    qkv_in,
    mix_own,
    mixbuf,
    stream,
    load_sems,
    push_send,
    push_recv,
    x_send,
    x_recv,
    i_send,
    r_send,
    a2a_send,
    a2a_recv,
    m_send,
    m_root,
    m_recv,
    out_send,
    out_recv,
    ready,
    turn,
):
    row_dev, blocks = table_ref.shape
    width = hid.shape[2]
    rows = nc * row_dev
    hd = keys.shape[2]
    heads = mix_own.shape[0]
    page_len = pool.shape[1]
    span = page_len * blocks
    wide = keys.shape[1]
    kvh = wide // row_dev // span
    per_chip = heads // nc
    part = wkv.shape[0]
    half = nc // 2
    parent = relay_tree(half)
    kids = {d: sorted((c for c in parent if parent[c] == d), reverse=True) for d in range(half + 1)}
    far = half // 2
    near = [(s, d) for d in range(far, 0, -1) for s in (1, -1)] + [(1, 0)]

    me = lax.axis_index("tensor")
    sec = lax.axis_index("section")
    z = me // 2
    core = lax.rem(me, 2)
    last = nsec - 1
    flip = lax.rem(sec, 2)
    piece = lax.rem(core + flip, 2)

    def dev(zz, s=None):
        where = {"tensor": lax.rem(zz + 2 * nc, nc) * 2 + core}
        if s is not None:
            where["section"] = s
        return where

    def ahead(zz):
        return {"tensor": lax.rem(zz + 2 * nc, nc) * 2 + 1 - core, "section": sec + 1}

    def behind(zz):
        return {"tensor": lax.rem(zz + 2 * nc, nc) * 2 + 1 - core, "section": sec - 1}

    def put(src, dst, ssem, rsem, where):
        copy = pltpu.make_async_remote_copy(
            src_ref=src, dst_ref=dst, send_sem=ssem, recv_sem=rsem, device_id=where, device_id_type=MESH
        )
        copy.start()
        return copy

    def wait_for(ref, sem):
        pltpu.make_async_copy(ref, ref, sem).wait()

    def cut(ref, axis, c):
        n = ref.shape[axis] // 2
        at = pl.multiple_of(c * n, n)
        return ref.at[pl.ds(at, n)] if axis == 0 else ref.at[:, pl.ds(at, n)]

    def shares(c):
        return [hid.at[c], bias.at[c], cut(wq, 1, c), cut(wkv, 0, c), cut(wo, 1, c)]

    sources = [hidden_hbm, bias_hbm, wq_hbm, wkv_hbm, wo_hbm]

    def load(k, src, dst):
        copy = pltpu.make_async_copy(src, dst, load_sems.at[k])
        copy.start()
        return copy

    load_gain, load_pool = load(0, gain_hbm, gain_in), load(1, pool_hbm, pool)
    own_loads = [load(2 + k, src, dst) for k, (src, dst) in enumerate(zip(sources, shares(core)))]

    barrier = pltpu.get_barrier_semaphore()

    def greet(where):
        pl.semaphore_signal(barrier, inc=1, device_id=where, device_id_type=MESH)

    sibling = {"tensor": z * 2 + 1 - core}
    greet(sibling)

    @pl.loop(1, nc)
    def _(i):
        greet(dev(z + i))

    @pl.when(sec < last)
    def _():
        for s, d in near:
            greet(ahead(z + s * d))

    @pl.when(sec > 0)
    def _():
        pl.semaphore_wait(barrier, nc + len(near))
        for s, d in near:
            pl.semaphore_signal(ready, inc=1, device_id=behind(z - s * d), device_id_type=MESH)

    @pl.when(sec == 0)
    def _():
        pl.semaphore_wait(barrier, nc)

    pushes = [
        put(src, dst, push_send.at[k], push_recv.at[k], sibling)
        for k, (src, dst) in enumerate(zip(sources, shares(core)))
    ]

    def send_stream(src, sems):
        return [put(src, xbuf.at[z], sems.at[k], x_recv.at[z], ahead(z + s * d)) for k, (s, d) in enumerate(near)]

    own_loads[0].wait()
    wait_for(hid.at[0], push_recv.at[0])

    @pl.when(jnp.logical_and(sec == 0, core == 1))
    def _():
        pl.semaphore_wait(turn, 1)

    @pl.when(sec == 0)
    def _():
        whole = 2 * rows
        at = lax.broadcasted_iota(jnp.int32, (rows, whole), 0)
        col = lax.broadcasted_iota(jnp.int32, (rows, whole), 1)
        row = (at // row_dev * 2 + core) * row_dev + lax.rem(at, row_dev)
        pick = jnp.where(col == row, 1.0, 0.0).astype(BF16)
        for c in range(2):
            first[c] = jnp.dot(pick, hid[c], preferred_element_type=F32).astype(BF16)
        for k, (s, d) in enumerate(near):
            if d:
                put(first, xbuf.at[z], i_send.at[k], x_recv.at[z], dev(z + s * d))
            else:
                pltpu.make_async_copy(first, xbuf.at[z], x_recv.at[z]).start()

    load_gain.wait()
    for t in range(2 * nc):
        gain[t] = gain_in[:, t * width : (t + 1) * width].astype(F32)
    load_pool.wait()
    for r in range(row_dev):
        for b in range(blocks):
            page = pool[lax.rem(table_ref[r, b], pool.shape[0])]
            for k in range(kvh):
                at = (r * kvh + k) * span + b * page_len
                keys[0, at : at + page_len, :] = page[:, k * hd : (k + 1) * hd]
                values[0, at : at + page_len, :] = page[:, (kvh + k) * hd : (kvh + k + 1) * hd]

    q_rows = per_chip * rows
    lane = lax.broadcasted_iota(jnp.int32, (q_rows, hd), 1)
    sample = lax.rem(lax.broadcasted_iota(jnp.int32, (q_rows, hd), 0), row_dev)
    position = jnp.full((q_rows, hd), len_ref[0], jnp.int32)
    for r in range(1, row_dev):
        position = jnp.where(sample == r, len_ref[r], position)
    position = position.astype(F32)
    frequency = jnp.exp(lax.rem(lane, hd // 2).astype(F32) * (-2.0 * LOG_ROPE_BASE / hd))
    angle = position * frequency
    sine = jnp.sin(angle)
    cos_tab[0] = jnp.cos(angle)
    sin_tab[0] = jnp.where(lane < hd // 2, -sine, sine)
    lim_tab[0] = position
    tables = [keys, values, cos_tab, sin_tab, lim_tab]

    @pl.when(flip == 1)
    def _():
        for k, table in enumerate(tables):
            put(table.at[0], table.at[1], push_send.at[len(sources) + k], push_recv.at[len(sources) + k], sibling)

    for k in range(1, 4):
        own_loads[k].wait()
        wait_for(shares(0)[k], push_recv.at[k])

    def chip_at(d, s):
        return lax.rem(z - s * d + nc, nc)

    def in_half(ref, s):
        n = ref.shape[0] // 2
        return ref.at[pl.ds(0 if s == 1 else n, n)]

    ring = [(far, 1), (far, -1)]
    ring += [(d, s) for d in range(1, half) if d != far for s in (1, -1)] + [(half, 1)]

    def pass_turn():
        @pl.when(jnp.logical_and(sec == 0, core == 0))
        def _():
            pl.semaphore_signal(turn, inc=1, device_id=sibling, device_id_type=MESH)

    def relay(place, recv, sems, items, direct, use, after_far=None):
        sent, passed = [], []
        for d, s in items:
            chip = chip_at(d, s)
            block = place(chip)
            wait_for(block, recv.at[chip])
            if d != far and passed:
                if after_far:
                    after_far()
                    after_far = None
                use(passed)
                passed = []
            passed.append(chip)
            for c in kids[d] if (d, s) not in direct else []:
                piece = in_half(block, s) if c == half else block
                sent.append(put(piece, piece, sems.at[len(sent)], recv.at[chip], dev(z + s * (c - d))))
        use(passed)
        return sent

    sums = {
        "q": jnp.zeros((rows, per_chip * hd), F32),
        "kv": jnp.zeros((rows, part), F32),
        "squares": jnp.zeros((rows, width), F32),
    }

    def project(chips):
        for chip in chips:
            project_one(chip)

    def project_one(chip):
        parts = []
        for c in range(2):
            x = xbuf[chip, c].astype(F32)
            sums["squares"] += x * x
            parts.append((x * gain[chip * 2 + c]).astype(BF16))
        y = jnp.concatenate(parts, axis=1)
        at = pl.multiple_of(chip * 2 * width, 2 * width)
        sums["q"] += jnp.dot(y, wq[pl.ds(at, 2 * width), :], preferred_element_type=F32)
        sums["kv"] += lax.dot_general(
            y, wkv[:, pl.ds(at, 2 * width)], (((1,), (1,)), ((), ())), preferred_element_type=F32
        )

    x_sent = relay(
        lambda c: xbuf.at[c], x_recv, x_send, ring[:2] + [(0, 1)] + ring[2:], [(0, 1)], project, pass_turn
    )

    def mine(ref, c):
        return ref.at[:, pl.ds(c * row_dev, row_dev)]

    scale = lax.rsqrt(jnp.sum(sums["squares"], axis=1, keepdims=True) / (2 * nc * width) + EPSILON)
    for i in range(per_chip):
        q = sums["q"][:, i * hd : (i + 1) * hd] * scale + bias[i].astype(F32)
        qkv_out[i] = q.astype(BF16)
    kv = (sums["kv"] * scale).astype(BF16).astype(F32)
    kv = jnp.concatenate([kv, jnp.zeros((rows, hd - part), F32)], axis=1)
    kv = pltpu.roll(kv, lax.rem(z, hd // part) * part, 1)
    qkv_out[per_chip] = kv.astype(BF16)

    for i in range(nc - 1):
        c = lax.rem(z + half + (1 - 2 * (i % 2)) * ((i + 1) // 2) + nc, nc)
        put(mine(qkv_out, c), mine(qkv_in, z), a2a_send, a2a_recv, dev(c))

    pltpu.make_async_copy(mine(qkv_out, z), mine(qkv_in, z), a2a_recv).start()

    @pl.when(flip == 1)
    def _():
        for k, table in enumerate(tables):
            wait_for(table.at[1], push_recv.at[len(sources) + k])

    def grid(shape, axis):
        return lax.broadcasted_iota(jnp.int32, shape, axis)

    group = heads // kvh
    q_of, c_of = grid((q_rows, wide), 0), grid((q_rows, wide), 1)
    key_head = (lax.rem(q_of, rows) // row_dev * per_chip + q_of // rows) // group
    matching = c_of // span == lax.rem(q_of, row_dev) * kvh + key_head
    usable = matching & (lax.rem(c_of, span).astype(F32) < lim_tab[flip][:, :1])
    s_row, s_col = grid((q_rows, rows), 0), grid((q_rows, rows), 1)
    same = lax.rem(s_row, row_dev) == lax.rem(s_col, row_dev)
    source = s_col // row_dev // (hd // part)
    wanted = (lax.rem(s_row, rows) // row_dev * per_chip + s_row // rows) // group
    pick_key = jnp.where(same & (source == wanted), 1.0, 0.0).astype(BF16)
    pick_value = jnp.where(same & (source == wanted + kvh), 1.0, 0.0).astype(BF16)
    root = hd ** (-0.5)
    cos, sin = cos_tab[flip], sin_tab[flip]
    wait_for(qkv_in, a2a_recv)

    def rotate(v):
        return (v * cos + pltpu.roll(v, hd // 2, 1) * sin).astype(BF16)

    rotated = rotate(jnp.concatenate([qkv_in[i].astype(F32) for i in range(per_chip)], axis=0))
    fresh = qkv_in[per_chip]
    key_new = rotate(jnp.dot(pick_key, fresh, preferred_element_type=F32))
    value_new = jnp.dot(pick_value, fresh, preferred_element_type=F32)
    scores = lax.dot_general(rotated, keys[flip], (((1,), (1,)), ((), ())), preferred_element_type=F32) * root
    own_score = jnp.sum(rotated.astype(F32) * key_new.astype(F32), axis=1, keepdims=True) * root
    top = jnp.maximum(jnp.max(jnp.where(usable, scores, -1e30), axis=1, keepdims=True), own_score)
    weights = jnp.where(usable, jnp.exp(scores - top), 0.0)
    own_weight = jnp.exp(own_score - top)
    total = jnp.sum(weights, axis=1, keepdims=True) + own_weight
    weights = (weights / total).astype(BF16)
    own_weight = (own_weight / total).astype(BF16).astype(F32)
    mixture = jnp.dot(weights, values[flip], preferred_element_type=F32) + own_weight * value_new
    mix_own[...] = mixture.astype(BF16).reshape(heads, row_dev, hd)

    def mix_place(c):
        return mixbuf.at[:, c]

    m_sent = []
    for c in kids[0]:
        for s in (1, -1):
            m_sent.append(put(mix_own, mix_place(z), m_root.at[len(m_sent)], m_recv.at[z], dev(z + s * c)))
    pltpu.make_async_copy(mix_own, mix_place(z), m_recv.at[z]).start()
    m_sent += relay(mix_place, m_recv, m_send, ring, [], lambda chips: None)
    wait_for(mix_place(z), m_recv.at[z])

    own_loads[4].wait()
    wait_for(shares(0)[4], push_recv.at[4])

    mixed = [mixbuf[i * nc + c].reshape(rows, hd) for c in range(nc) for i in range(per_chip)]
    change = jnp.dot(jnp.concatenate(mixed, axis=1), wo[...], preferred_element_type=F32)
    for c in range(2):
        x = xbuf[z, c].astype(F32)
        stream[c] = (x + change[:, c * width : (c + 1) * width]).astype(BF16)

    chips = nc // nsec

    @pl.when(sec < last)
    def _():
        pl.semaphore_wait(ready, len(near))
        for copy in send_stream(stream, r_send):
            copy.wait_send()

    @pl.when(sec == last)
    def _():
        def share(s, c, j):
            return (
                stream.at[c, pl.ds((s * chips + j) * row_dev, row_dev)],
                out_ref.at[pl.ds((j * 2 + piece) * row_dev, row_dev)],
            )

        def sem_of(s, c, j):
            return out_send.at[(j * 2 + c) * nsec + s]

        for j in range(chips):
            for c in range(2):

                @pl.loop(0, last)
                def _(s):
                    put(*share(s, c, j), sem_of(s, c, j), out_recv, {"section": s, "tensor": z * 2 + c})

                @pl.when(core == c)
                def _():
                    pltpu.make_async_copy(*share(last, c, j), out_recv).start()

                @pl.when(core != c)
                def _():
                    put(*share(last, c, j), sem_of(last, c, j), out_recv, sibling)

        for j in range(chips):
            for c in range(2):

                @pl.loop(0, last)
                def _(s):
                    wait_for(stream.at[0, pl.ds(0, row_dev)], sem_of(s, c, j))

                @pl.when(core != c)
                def _():
                    wait_for(stream.at[0, pl.ds(0, row_dev)], sem_of(last, c, j))

    @pl.when(sec == 0)
    def _():
        for k, (s, d) in enumerate(near):
            if d:
                wait_for(first, i_send.at[k])

    @pl.when(flip == 1)
    def _():
        for k, table in enumerate(tables):
            wait_for(table.at[0], push_send.at[len(sources) + k])

    others = pl.ds(0, rows - row_dev)
    wait_for(qkv_out.at[:, others], a2a_send)
    for copy in pushes + x_sent + m_sent:
        copy.wait_send()
    wait_for(out_ref, out_recv)


def solution(mesh):
    nc, nsec = mesh.shape["tensor"] // 2, mesh.shape["section"]

    def step(hidden, norm_gain, query_weight, query_bias, kv_weight, out_weight, kv_pool, page_table, context_len):
        all_rows, width = hidden.shape
        features, hd = query_weight.shape[1:]
        pages, page_len, kv_width = kv_pool.shape[1:]
        row_dev, blocks = page_table.shape
        part = 2 * kv_weight.shape[2]
        kvh = kv_width // (2 * hd)
        cached = row_dev * kvh * blocks * page_len
        heads = 2 * nc
        rows = all_rows // 2
        q_rows = rows * heads // nc
        anywhere = pl.BlockSpec(memory_space=pl.ANY)
        scalars = pl.BlockSpec(memory_space=pltpu.SMEM)
        dma = pltpu.SemaphoreType.DMA
        vmem = pltpu.VMEM
        return pl.pallas_call(
            functools.partial(kernel, nc, nsec),
            out_shape=jax.ShapeDtypeStruct((all_rows // nsec, width), BF16),
            in_specs=[anywhere] * 7 + [scalars] * 2,
            out_specs=pl.BlockSpec(memory_space=vmem),
            scratch_shapes=[
                vmem((2, all_rows, width), BF16),
                vmem((1, features), BF16),
                vmem((2 * nc, 1, width), F32),
                vmem((features, 2 * hd), BF16),
                vmem((2, 1, hd), BF16),
                vmem((part, features), BF16),
                vmem((heads * hd, 2 * width), BF16),
                vmem((pages, page_len, kv_width), BF16),
                vmem((2, cached, hd), BF16),
                vmem((2, cached, hd), BF16),
                vmem((2, q_rows, hd), F32),
                vmem((2, q_rows, hd), F32),
                vmem((2, q_rows, hd), F32),
                vmem((2, rows, width), BF16),
                vmem((nc, 2, rows, width), BF16),
                vmem((3, rows, hd), BF16),
                vmem((3, rows, hd), BF16),
                vmem((heads, row_dev, hd), BF16),
                vmem((heads, nc, row_dev, hd), BF16),
                vmem((2, rows, width), BF16),
                dma((7,)),
                dma((10,)),
                dma((10,)),
                dma((2 * nc,)),
                dma((nc,)),
                dma((nc,)),
                dma((nc,)),
                dma,
                dma,
                dma((2 * nc,)),
                dma((2 * nc,)),
                dma((nc,)),
                dma((2 * nc,)),
                dma,
                pltpu.SemaphoreType.REGULAR,
                pltpu.SemaphoreType.REGULAR,
            ],
            compiler_params=pltpu.CompilerParams(collective_id=0, has_side_effects=True),
        )(
            hidden,
            norm_gain,
            query_weight[0],
            query_bias,
            kv_weight[0].T,
            out_weight[0],
            kv_pool[0],
            page_table,
            context_len,
        )

    tensor = "tensor"
    return jax.shard_map(
        step,
        mesh=mesh,
        in_specs=(
            P("groups", tensor),
            P("section", None),
            P("section", None, tensor),
            P("section", tensor),
            P("section", None, tensor),
            P("section", None, tensor),
            P("section", ("groups", tensor), None, None),
            P(("groups", tensor), None),
            P(("groups", tensor)),
        ),
        out_specs=P(("groups", "section"), tensor),
        check_vma=False,
    )
```
